8 devices in a mesh: rep: 1 (over z), dp: 8 (over x, y, core).
Axes of the slice: x: 2, y: 2, z: 1, core: 2. Of those that a mesh axis runs over, the one named last changes fastest.
Arguments:
- x: bfloat16 [8, 2048, 896], P(('rep', 'dp'))
- dy: bfloat16 [8, 2048, 896], P(('rep', 'dp'))
- w_gate: bfloat16 [2, 896, 2560], replicated
- w_up: bfloat16 [2, 896, 2560], replicated
- w_down: bfloat16 [2, 2560, 896], replicated
- m_w_gate: float32 [2, 896, 2560], P(None, 'dp')
- m_w_up: float32 [2, 896, 2560], P(None, 'dp')
- m_w_down: float32 [2, 2560, 896], P(None, 'dp')
- v_w_gate: float32 [2, 896, 2560], P(None, 'dp')
- v_w_up: float32 [2, 896, 2560], P(None, 'dp')
- v_w_down: float32 [2, 2560, 896], P(None, 'dp')
Outputs:
- output 1: bfloat16 [2, 896, 2560], P('rep')
- output 2: bfloat16 [2, 896, 2560], P('rep')
- output 3: bfloat16 [2, 2560, 896], P('rep')
- output 4: float32 [2, 896, 2560], P('rep', 'dp')
- output 5: float32 [2, 896, 2560], P('rep', 'dp')
- output 6: float32 [2, 2560, 896], P('rep', 'dp')
- output 7: float32 [2, 896, 2560], P('rep', 'dp')
- output 8: float32 [2, 896, 2560], P('rep', 'dp')
- output 9: float32 [2, 2560, 896], P('rep', 'dp')
All inputs are finite; a program needn't handle non-finite values.
Results may differ from the reference program's by a relative error of at most 0.022.
Values are sent between devices in bfloat16 or wider.
A program may use at most 2 GiB of HBM per device.

```python
import jax
import jax.numpy as jnp
from jax import lax

SEQUENCES = 8
TOKENS = 2048
D = 896
FF = 2560
LAYERS = 2
NAMES = ("w_gate", "w_up", "w_down")
SHAPES = {"w_gate": (LAYERS, D, FF), "w_up": (LAYERS, D, FF), "w_down": (LAYERS, FF, D)}


def bump(key, n, height):
    away = (jnp.arange(n, dtype=jnp.int32) - jax.random.randint(key, (), 0, n, jnp.int32)) % n
    return jnp.where(away < n // 8, height, 1.0)


def together(key, own, strength):
    shared = jax.random.normal(key, own.shape[1:], jnp.float32)
    return (own + strength * shared) * lax.rsqrt(1 + strength * strength)


def setup_inputs(seed: int = 0, part: int = 0) -> dict:
    kx, kdy, ka, kb, kz, kf, kh, kl, *keys = jax.random.split(jax.random.key(seed), 8 + 3 * len(NAMES))
    kx, kdy, ka, kb = (jax.random.fold_in(k, part) for k in (kx, kdy, ka, kb))
    kw, km, kv = (keys[i::3] for i in range(3))
    shape = (SEQUENCES, TOKENS, D)
    much_x, much_dy = jax.random.uniform(kz, (2,), jnp.float32, 0.0, 1.0)
    loud = 2.0 ** jax.random.uniform(jax.random.fold_in(kz, 1), (), jnp.float32, -1.0, 2.0)
    layers = 2.0 ** jax.random.uniform(kl, (LAYERS, 1, 1), jnp.float32, -1.0, 1.0)
    x = together(ka, jax.random.normal(kx, shape, jnp.float32), much_x) * bump(kf, D, 4.0)
    dy = together(kb, jax.random.normal(kdy, shape, jnp.float32), much_dy)
    drawn = {"x": x.astype(jnp.bfloat16), "dy": (loud * dy * (SEQUENCES * TOKENS) ** -0.5).astype(jnp.bfloat16)}
    for key, name in zip(kw, NAMES, strict=True):
        w = jax.random.normal(key, SHAPES[name], jnp.float32) * SHAPES[name][1] ** -0.5
        drawn[name] = (w * {"w_gate": 1.0, "w_up": bump(kh, FF, 4.0), "w_down": layers}[name]).astype(jnp.bfloat16)
    for key, name in zip(km, NAMES, strict=True):
        drawn[f"m_{name}"] = 0.1 * jax.random.normal(key, SHAPES[name], jnp.float32)
    for key, name in zip(kv, NAMES, strict=True):
        drawn[f"v_{name}"] = jax.random.uniform(key, SHAPES[name], jnp.float32, 0.005, 0.015)
    return drawn


def matmul(a, w):
    return jnp.dot(a, w, preferred_element_type=jnp.float32).astype(jnp.bfloat16)


def normed(h):
    wide = h.astype(jnp.float32)
    scale = lax.rsqrt(jnp.mean(wide**2, -1, keepdims=True) + 1e-6)
    return (wide * scale).astype(jnp.bfloat16)


def layer(h, w):
    a = normed(h)
    gate = jnp.dot(a, w["w_gate"], preferred_element_type=jnp.float32)
    up = jnp.dot(a, w["w_up"], preferred_element_type=jnp.float32)
    return h + matmul((jax.nn.silu(gate) * up).astype(jnp.bfloat16), w["w_down"])


def adamw(w, m, v, g):
    m = 0.9 * m + 0.1 * g
    v = 0.95 * v + 0.05 * g * g
    step = m * lax.rsqrt(v + 1e-8) + 0.1 * w
    return (w - 0.02 * step).astype(jnp.bfloat16), m, v


def clipped(gradients, sum_of_squares, count):
    factor = jnp.minimum(1.0, 0.5 * lax.rsqrt(sum_of_squares / count + 1e-30))
    return [g * factor for g in gradients]


def stack(weights, h):
    return lax.scan(lambda h, w: (layer(h, w), None), h, weights)[0]


def reference(x, dy, w_gate, w_up, w_down, m_w_gate, m_w_up, m_w_down, v_w_gate, v_w_up, v_w_down):
    weights = dict(zip(NAMES, (w_gate, w_up, w_down), strict=True))

    def take(so_far, sequence):
        h, by_y = sequence
        _, back = jax.vjp(lambda w: stack(w, h), weights)
        return jax.tree.map(lambda total, term: total + term.astype(jnp.float32), so_far, back(by_y)[0]), None

    none_yet = {name: jnp.zeros(w.shape, jnp.float32) for name, w in weights.items()}
    by_weights, _ = lax.scan(take, none_yet, (x, dy))
    gradients = [by_weights[name].astype(jnp.bfloat16).astype(jnp.float32) for name in NAMES]
    gradients = clipped(gradients, sum(jnp.sum(g * g) for g in gradients), sum(g.size for g in gradients))
    new = [
        adamw(w.astype(jnp.float32), m, v, g)
        for w, m, v, g in zip((w_gate, w_up, w_down), (m_w_gate, m_w_up, m_w_down), (v_w_gate, v_w_up, v_w_down), gradients, strict=True)
    ]
    return tuple(one[which] for which in range(3) for one in new)
```

```python
import functools

import jax
import jax.numpy as jnp
from jax import lax
from jax.experimental import pallas as pl
from jax.experimental.pallas import tpu as pltpu
from jax.sharding import PartitionSpec as P

F32, BF = jnp.float32, jnp.bfloat16
VMEM = 62 * 1024 * 1024
X, Y, CORE = 4, 2, 1


def dot(a, b, ca=1, cb=0):
    return lax.dot_general(a, b, (((ca,), (cb,)), ((), ())), preferred_element_type=F32)


def norm_scale(wide):
    return lax.rsqrt(jnp.mean(wide * wide, -1, keepdims=True) + 1e-6)


def whole(shape):
    return pl.BlockSpec(shape, lambda i, *_: (0,) * len(shape), pipeline_mode=pl.Buffered(1))


def sds(shape, dtype):
    return jax.ShapeDtypeStruct(shape, dtype)


def params():
    return pltpu.CompilerParams(vmem_limit_bytes=VMEM)


def cost(matmuls, n, d, ff, bytes_accessed):
    return pl.CostEstimate(flops=2 * matmuls * n * d * ff, bytes_accessed=bytes_accessed, transcendentals=0)


def forward_kernel(chunk, down, h_ref, wg_ref, wu_ref, *refs):
    if down:
        wd_ref, a_ref, act_ref, sa_ref, sb_ref, h1_ref = refs
    else:
        a_ref, act_ref, sa_ref, sb_ref = refs
    wide = h_ref[...].astype(F32)
    a = (wide * norm_scale(wide)).astype(BF)
    a_ref[...] = a
    for c in range(wg_ref.shape[1] // chunk):
        s = pl.ds(c * chunk, chunk)
        gate, up = dot(a, wg_ref[:, s]), dot(a, wu_ref[:, s])
        sig = 1.0 / (1.0 + jnp.exp(-gate))
        silu = gate * sig
        act_ref[:, s] = (silu * up).astype(BF)
        sb_ref[:, s] = silu
        sa_ref[:, s] = up * (sig + silu * (1.0 - sig))
    if down:
        out = dot(act_ref[...], wd_ref[...]).astype(BF)
        h1_ref[...] = (h_ref[...].astype(F32) + out.astype(F32)).astype(BF)


def forward(h, wg, wu, wd=None, tile=256, chunk=1280):
    n, d = h.shape
    ff = wg.shape[1]
    row = lambda w: pl.BlockSpec((tile, w), lambda i: (i, 0))
    down = wd is not None
    return pl.pallas_call(
        functools.partial(forward_kernel, chunk, down),
        grid=(n // tile,),
        in_specs=[row(d), whole((d, ff)), whole((d, ff))] + [whole((ff, d))] * down,
        out_specs=[row(d), row(ff), row(ff), row(ff)] + [row(d)] * down,
        out_shape=[sds((n, d), BF), sds((n, ff), BF), sds((n, ff), F32), sds((n, ff), F32)] + [sds((n, d), BF)] * down,
        compiler_params=params(),
        cost_estimate=cost(3 if down else 2, n, d, ff, 10 * n * ff),
        name="forward",
    )(h, wg, wu, *([wd] if down else []))


def down_grad_kernel(s_ref, act_ref, dy_ref, keep_ref, send_ref):
    g = dot(act_ref[...], dy_ref[...], 0, 0)
    rows = g.shape[0] // 2
    first, second = g[:rows], g[rows:]
    mine = s_ref[1] == 0
    keep_ref[0] = jnp.where(mine, first, second).astype(BF)
    send_ref[0] = jnp.where(mine, second, first).astype(BF)


def down_grad(where, act, dy):
    n, ff = act.shape
    d = dy.shape[1]
    out = pl.BlockSpec((1, ff // 8, d), lambda i, s: (i, 0, 0))
    return pl.pallas_call(
        down_grad_kernel,
        grid_spec=pltpu.PrefetchScalarGridSpec(
            num_scalar_prefetch=1,
            grid=(4,),
            in_specs=[pl.BlockSpec((n, ff // 4), lambda i, s: (0, i ^ s[0])), whole((n, d))],
            out_specs=[out, out],
        ),
        out_shape=[sds((4, ff // 8, d), BF)] * 2,
        compiler_params=params(),
        cost_estimate=cost(1, n, d, ff, 2 * n * ff),
        name="down_grad",
    )(where, act, dy)


def up_grad_kernel(chunk, full, s_ref, a_ref, dy_ref, sa_ref, sb_ref, wd_ref, *refs):
    gk_ref, gs_ref, uk_ref, us_ref, dg_ref, du_ref = refs
    n, d = a_ref.shape

    def body(t, _):
        r = pl.ds(pl.multiple_of(t * chunk, chunk), chunk)
        dp = dot(dy_ref[r, :], wd_ref[...], 1, 1).astype(BF).astype(F32)
        du_ref[r, :] = (dp * sb_ref[r, :]).astype(BF)
        dg_ref[r, :] = (dp * sa_ref[r, :]).astype(BF)
        return 0

    lax.fori_loop(0, n // chunk, body, 0)
    rows = d // 8
    mine = s_ref[1] == 0
    for by_ref, keep_ref, send_ref in ((dg_ref, gk_ref, gs_ref), (du_ref, uk_ref, us_ref)):
        g = dot(a_ref[...], by_ref[...], 0, 0)
        for q in range(4):
            first, second = (g[(2 * q + i) * rows : (2 * q + i + 1) * rows] for i in (0, 1))
            slot = q ^ s_ref[0]
            keep_ref[slot] = jnp.where(mine, first, second).astype(BF)
            send_ref[slot] = jnp.where(mine, second, first).astype(BF)


def up_grad(where, a, dy, sa, sb, wd, first, last, full, tile=512, chunk=512):
    n, d = a.shape
    width = (last - first) * tile
    cols = pl.BlockSpec((n, tile), lambda j, s: (0, j + first))
    out = pl.BlockSpec((4, d // 8, tile), lambda j, s: (0, 0, j))
    by = pl.BlockSpec((n, tile), lambda j, s: (0, j))
    results = pl.pallas_call(
        functools.partial(up_grad_kernel, chunk, full),
        grid_spec=pltpu.PrefetchScalarGridSpec(
            num_scalar_prefetch=1,
            grid=(last - first,),
            in_specs=[whole((n, d)), whole((n, d)), cols, cols, pl.BlockSpec((tile, d), lambda j, s: (j + first, 0))],
            out_specs=[out] * 4 + [by] * (2 * full),
            scratch_shapes=[pltpu.VMEM((n, tile), BF)] * (2 * (not full)),
        ),
        out_shape=[sds((4, d // 8, width), BF)] * 4 + [sds((n, width), BF)] * (2 * full),
        compiler_params=params(),
        cost_estimate=cost(3, n, d, width, 8 * n * width),
        name="up_grad",
    )(where, a, dy, sa, sb, wd)
    return results[0:2], results[2:4], results[4:]


def state_grad_kernel(h_ref, dy_ref, dg_ref, du_ref, wg_ref, wu_ref, dh_ref):
    da = dot(dg_ref[...], wg_ref[...], 1, 1) + dot(du_ref[...], wu_ref[...], 1, 1)
    da = da.astype(BF).astype(F32)
    wide = h_ref[...].astype(F32)
    s = norm_scale(wide)
    dx = s * (da - wide * (s * s * jnp.mean(da * wide, -1, keepdims=True)))
    dh_ref[...] = (dy_ref[...].astype(F32) + dx.astype(BF).astype(F32)).astype(BF)


def state_grad(h, dy, dg, du, wg, wu, tile=512):
    n, d = h.shape
    ff = wg.shape[1]
    row = lambda w: pl.BlockSpec((tile, w), lambda i: (i, 0))
    return pl.pallas_call(
        state_grad_kernel,
        grid=(n // tile,),
        in_specs=[row(d), row(d), row(ff), row(ff), whole((d, ff)), whole((d, ff))],
        out_specs=row(d),
        out_shape=sds((n, d), BF),
        compiler_params=params(),
        cost_estimate=cost(2, n, d, ff, 4 * n * ff),
        name="state_grad",
    )(h, dy, dg, du, wg, wu)


def swap(value, bit):
    return lax.ppermute(value, "dp", [(i, i ^ bit) for i in range(8)])


def add(*terms):
    return sum(t.astype(F32) for t in terms)


def reduce_scatter(keep, send, axis):
    got = swap(send, CORE)
    half = keep.shape[axis] // 2
    cut = lambda t, which: lax.slice_in_dim(t, which * half, (which + 1) * half, axis=axis - 4)
    ka, kb, ga, gb = cut(keep, 0), cut(keep, 1), cut(got, 0), cut(got, 1)
    xa = swap(add(ka[1], ga[1]).astype(BF), X)
    yb = swap(add(kb[:, 1], gb[:, 1]).astype(BF), Y)
    ya = swap(add(ka[0, 1], ga[0, 1], xa[1]).astype(BF), Y)
    xb = swap(add(kb[1, 0], gb[1, 0], yb[1]).astype(BF), X)
    a = add(ka[0, 0], ga[0, 0], xa[0], ya)
    b = add(kb[0, 0], gb[0, 0], yb[0], xb)
    return jnp.concatenate([a, b], axis=axis - 2).astype(BF)


def all_gather(mine):
    layers, rows, columns = mine.shape
    half = rows // 32 * 16
    me = lax.axis_index("dp")
    by_x, by_y = swap(mine, X), swap(mine, Y)
    far_a, far_b = swap(by_x[:, :half], Y), swap(by_y[:, half:], X)
    out = jnp.zeros((layers, 8 * rows, columns), mine.dtype)
    for bit, off, block in ((0, 0, mine), (X, 0, by_x), (Y, 0, by_y), (X ^ Y, 0, far_a), (X ^ Y, half, far_b)):
        for core, part in ((0, block), (CORE, swap(block, CORE))):
            out = lax.dynamic_update_slice(out, part, (0, (me ^ bit ^ core) * rows + off, 0))
    return out


def adamw(w, m, v, g):
    m = 0.9 * m + 0.1 * g
    v = 0.95 * v + 0.05 * g * g
    step = m * lax.rsqrt(v + 1e-8) + 0.1 * w
    return (w - 0.02 * step).astype(BF), m, v


def solution(mesh):
    def step(x, dy, *arrays):
        weights, ms, vs = (arrays[i : i + 3] for i in (0, 3, 6))
        (wg0, wg1), (wu0, wu1), (wd0, wd1) = ((w[0], w[1]) for w in weights)
        h0, dy = x[0], dy[0]
        me = lax.axis_index("dp")
        where = jnp.stack([me // 2, me % 2]).astype(jnp.int32)
        four = lambda t: t.reshape(2, 2, *t.shape[1:])
        scatter = lambda pair, axis: reduce_scatter(*map(four, pair), axis)

        a0, act0, sa0, sb0, h1 = forward(h0, wg0, wu0, wd0)
        a1, act1, sa1, sb1 = forward(h1, wg1, wu1)
        down1 = scatter(down_grad(where, act1, dy), 2)
        tiles = wg0.shape[1] // 512
        gate1, up1, (dg, du) = up_grad(where, a1, dy, sa1, sb1, wd1, 0, tiles, True)
        gate1, up1 = scatter(gate1, 3), scatter(up1, 3)
        dh1 = state_grad(h1, dy, dg, du, wg1, wu1)
        down0 = scatter(down_grad(where, act0, dh1), 2)
        gate0, up0 = [], []
        for first, last in ((0, 3), (3, tiles)):
            gate, up, _ = up_grad(where, a0, dh1, sa0, sb0, wd0, first, last, False)
            gate0.append(scatter(gate, 3))
            up0.append(scatter(up, 3))
        gate0, up0 = (jnp.concatenate(t, axis=1) for t in (gate0, up0))

        gradients = [jnp.stack(t).astype(F32) for t in ((gate0, gate1), (up0, up1), (down0, down1))]
        squares = sum(jnp.sum(g * g) for g in gradients).reshape(1, 1)
        for bit in (CORE, Y, X):
            squares = squares + swap(squares, bit)
        count = sum(w.size for w in weights)
        factor = jnp.minimum(1.0, 0.5 * lax.rsqrt(squares[0, 0] / count + 1e-30))
        new = []
        for w, m, v, g in zip(weights, ms, vs, gradients, strict=True):
            mine = lax.dynamic_slice_in_dim(w, me * m.shape[1], m.shape[1], axis=1)
            new.append(adamw(mine.astype(F32), m, v, g * factor))
        return tuple(all_gather(w) for w, _, _ in new) + tuple(m for _, m, _ in new) + tuple(v for _, _, v in new)

    batch, rows = P(("rep", "dp")), P(None, "dp")
    return jax.shard_map(
        step,
        mesh=mesh,
        in_specs=(batch,) * 2 + (P(),) * 3 + (rows,) * 6,
        out_specs=(P("rep"),) * 3 + (P("rep", "dp"),) * 6,
        check_vma=False,
    )
```

```python
import functools

import jax
import jax.numpy as jnp
from jax import lax
from jax.experimental import pallas as pl
from jax.experimental.pallas import tpu as pltpu
from jax.sharding import PartitionSpec as P

F32, BF = jnp.float32, jnp.bfloat16
VMEM = 67043328
X, Y, CORE = 4, 2, 1


def dot(a, b, ca=1, cb=0):
    return lax.dot_general(a, b, (((ca,), (cb,)), ((), ())), preferred_element_type=F32)


def norm_scale(wide):
    return lax.rsqrt(jnp.mean(wide * wide, -1, keepdims=True) + 1e-6)


def whole(shape):
    return pl.BlockSpec(shape, lambda i, *_: (0,) * len(shape), pipeline_mode=pl.Buffered(1))


def sds(shape, dtype):
    return jax.ShapeDtypeStruct(shape, dtype)


def params():
    return pltpu.CompilerParams(vmem_limit_bytes=VMEM)


def cost(matmuls, n, d, ff, bytes_accessed):
    return pl.CostEstimate(flops=2 * matmuls * n * d * ff, bytes_accessed=bytes_accessed, transcendentals=0)


def forward_kernel(chunk, down, h_ref, wg_ref, wu_ref, *refs):
    if down:
        wd_ref, a_ref, act_ref, sa_ref, sb_ref, h1_ref = refs
    else:
        a_ref, act_ref, sa_ref, sb_ref = refs
    wide = h_ref[...].astype(F32)
    a = (wide * norm_scale(wide)).astype(BF)
    a_ref[...] = a
    for c in range(wg_ref.shape[1] // chunk):
        s = pl.ds(c * chunk, chunk)
        gate, up = dot(a, wg_ref[:, s]), dot(a, wu_ref[:, s])
        sig = 1.0 / (1.0 + jnp.exp(-gate))
        silu = gate * sig
        act_ref[:, s] = (silu * up).astype(BF)
        sb_ref[:, s] = silu
        sa_ref[:, s] = up * (sig + silu * (1.0 - sig))
    if down:
        out = dot(act_ref[...], wd_ref[...]).astype(BF)
        h1_ref[...] = (h_ref[...].astype(F32) + out.astype(F32)).astype(BF)


def forward(number, h, weights, down, tile=256, chunk=1280):
    n, d = h.shape
    ff = weights[0].shape[2]
    row = lambda w: pl.BlockSpec((tile, w), lambda i: (i, 0))
    of = lambda w: pl.BlockSpec((None, *w.shape[1:]), lambda i: (number, 0, 0), pipeline_mode=pl.Buffered(1))
    used = weights[: 2 + down]
    return pl.pallas_call(
        functools.partial(forward_kernel, chunk, down),
        grid=(n // tile,),
        in_specs=[row(d)] + [of(w) for w in used],
        out_specs=[row(d), row(ff), row(ff), row(ff)] + [row(d)] * down,
        out_shape=[sds((n, d), BF), sds((n, ff), BF), sds((n, ff), F32), sds((n, ff), F32)] + [sds((n, d), BF)] * down,
        compiler_params=params(),
        cost_estimate=cost(3 if down else 2, n, d, ff, 10 * n * ff),
        name="forward",
    )(h, *used)


def peers():
    me = lax.axis_index("dp")
    x, y, core = me // 4, me // 2 % 2, me % 2
    return (x, y, core), (me + 1 - 2 * core, me + 2 - 4 * y, me + 4 - 8 * x)


def xor(a, b):
    return a + b - 2 * a * b


def send(src, dst, sems, to):
    return pltpu.make_async_remote_copy(
        src_ref=src,
        dst_ref=dst,
        send_sem=sems[0],
        recv_sem=sems[1],
        device_id={"dp": to},
        device_id_type=pl.DeviceIdType.MESH,
    )


def total(*terms):
    return sum(t.astype(F32) for t in terms)


def backward_kernel(states, tokens, tile, steps, *refs):
    refs = list(refs)
    take = lambda k: [refs.pop(0) for _ in range(k)]
    a_ref, dy_ref, act_ref, sa_ref, sb_ref, wd_ref = take(6)
    if states:
        h_ref, wg_ref, wu_ref = take(3)
    gate_ref, up_ref, down_ref = take(3)
    if states:
        (dh_ref,) = take(1)
    dg_s, du_s = take(2)
    dk, do, di, da_sum, db_sum, dsx, dsy, drx, dry, dsy2, dsx2, dry2, drx2 = take(13)
    gk, go, gi, g_sum, gs1, gr1, gs2, gr2 = take(8)
    uk, uo, ui, u_sum, us1, ur1, us2, ur2 = take(8)
    d_core, d_link, p_core, p_link = take(4)
    if states:
        da_s, h_s, dh_s, h_sem, dh_sem = take(5)

    n, d = a_ref.shape
    parts = n // tokens
    i = pl.program_id(0)
    (x, y, core), (to_core, to_y, to_x) = peers()
    mine = core == 0

    def down_copy(q):
        sx, sy = xor(q // 2, x), xor(q % 2, y)
        return send(do.at[sx, sy], di.at[sx, sy], (d_core.at[0, q], d_core.at[1, q]), to_core)

    def link(sems, src, dst, to):
        return send(src, dst, sems, to)

    def down_links(stage):
        sem = lambda k: (d_link.at[0, k], d_link.at[1, k])
        if stage == 1:
            return send(dsx, drx, sem(0), to_x), send(dsy, dry, sem(1), to_y)
        return send(dsy2, dry2, sem(2), to_y), send(dsx2, drx2, sem(3), to_x)

    def core_copy(which, u):
        src, dst = ((go, gi), (uo, ui))[which]
        slot = u % 2
        return send(src, dst.at[slot], (p_core.at[0, which, slot], p_core.at[1, which, slot]), to_core)

    def pair_links(stage, u):
        sem = lambda k: (p_link.at[0, k, u], p_link.at[1, k, u])
        if stage == 1:
            return send(gs1, gr1.at[u], sem(0), to_x), send(us1, ur1.at[u], sem(1), to_y)
        return send(gs2.at[u % 2], gr2.at[u], sem(2), to_y), send(us2.at[u % 2], ur2.at[u], sem(3), to_x)

    def start(copies):
        for c in copies:
            c.start()

    def wait(copies):
        for c in copies:
            c.wait()

    half = dk.shape[2] // 2
    lo, hi = pl.ds(0, half), pl.ds(half, half)

    def down_first():
        wait([down_copy(q) for q in range(4)])
        dsx[...] = total(dk[1, :, lo], di[1, :, lo]).astype(BF)
        dsy[...] = total(dk[:, 1, hi], di[:, 1, hi]).astype(BF)
        start(down_links(1))
        da_sum[...] = total(dk[0, :, lo], di[0, :, lo])
        db_sum[...] = total(dk[:, 0, hi], di[:, 0, hi])

    def down_second():
        wait(down_links(1))
        dsy2[...] = total(da_sum[1], drx[1]).astype(BF)
        dsx2[...] = total(db_sum[1], dry[1]).astype(BF)
        start(down_links(2))
        da_sum[0] = total(da_sum[0], drx[0])
        db_sum[0] = total(db_sum[0], dry[0])

    def down_last():
        wait(down_links(2))
        down_ref[lo, :] = total(da_sum[0], dry2[...]).astype(BF)
        down_ref[hi, :] = total(db_sum[0], drx2[...]).astype(BF)

    def pair_first(u):
        slot = u % 2
        wait([core_copy(0, u), core_copy(1, u)])
        gs1[...] = total(gk[1], gi[slot, 1]).astype(BF)
        us1[...] = total(uk[:, 1], ui[slot, :, 1]).astype(BF)
        start(pair_links(1, u))
        g_sum[slot] = total(gk[0], gi[slot, 0])
        u_sum[slot] = total(uk[:, 0], ui[slot, :, 0])

    def pair_second(u):
        slot = u % 2
        wait(pair_links(1, u))
        gs2[slot] = total(g_sum[slot, 1], gr1[u, 1]).astype(BF)
        us2[slot] = total(u_sum[slot, 1], ur1[u, 1]).astype(BF)
        start(pair_links(2, u))
        g_sum[slot, 0] = total(g_sum[slot, 0], gr1[u, 0])
        u_sum[slot, 0] = total(u_sum[slot, 0], ur1[u, 0])

    def pair_last(u):
        slot = u % 2
        wait(pair_links(2, u))
        cols = pl.ds(pl.multiple_of(u * tile, tile), tile)
        gate_ref[:, cols] = total(g_sum[slot, 0], gr2[u]).astype(BF)
        up_ref[:, cols] = total(u_sum[slot, 0], ur2[u]).astype(BF)

    @pl.when(i == 0)
    def _():
        barrier = pltpu.get_barrier_semaphore()
        for to in (to_core, to_y, to_x):
            pl.semaphore_signal(barrier, inc=1, device_id={"dp": to}, device_id_type=pl.DeviceIdType.MESH)
        pl.semaphore_wait(barrier, 3)
        if states:

            def clear(t, _):
                da_s[pl.ds(pl.multiple_of(t * 256, 256), 256), :] = jnp.zeros((256, d), F32)
                return 0

            lax.fori_loop(0, n // 256, clear, 0)

    @pl.when(i < 4)
    def _():
        g = dot(act_ref[...], dy_ref[...], 0, 0)
        rows = g.shape[0] // 2
        sx, sy = xor(i // 2, x), xor(i % 2, y)
        dk[sx, sy] = jnp.where(mine, g[:rows], g[rows:]).astype(BF)
        do[sx, sy] = jnp.where(mine, g[rows:], g[:rows]).astype(BF)
        down_copy(i).start()

    @pl.when(i >= 4)
    def _():
        j, t = (i - 4) // parts, (i - 4) % parts
        r = pl.ds(pl.multiple_of(t * tokens, tokens), tokens)
        dp = dot(dy_ref[r, :], wd_ref[...], 1, 1).astype(BF).astype(F32)
        du = (dp * sb_ref[...]).astype(BF)
        dg = (dp * sa_ref[...]).astype(BF)
        dg_s[r, :], du_s[r, :] = dg, du
        if states:
            da_s[r, :] += dot(dg, wg_ref[...], 1, 1) + dot(du, wu_ref[...], 1, 1)

        @pl.when(t == parts - 1)
        def _():
            pl.when(j == 0)(down_first)
            pl.when(j == 2)(down_second)
            pl.when(j >= 2)(lambda: pair_second(j - 2))
            pl.when(j >= 3)(lambda: pair_last(j - 3))
            pl.when(j >= 1)(lambda: pair_first(j - 1))
            pl.when(j == 3)(down_last)
            rows = d // 8
            for which, (by, keep, out) in enumerate(((dg_s, gk, go), (du_s, uk, uo))):
                g = dot(a_ref[...], by[...], 0, 0)
                for q in range(4):
                    first, second = (g[(2 * q + e) * rows : (2 * q + e + 1) * rows] for e in (0, 1))
                    sx, sy = xor(q // 2, x), xor(q % 2, y)
                    keep[sx, sy] = jnp.where(mine, first, second).astype(BF)
                    out[sx, sy] = jnp.where(mine, second, first).astype(BF)
                core_copy(which, j).start()

    @pl.when(i == 4 + steps * parts - 1)
    def _():
        pair_second(steps - 2)
        pair_last(steps - 3)
        pair_first(steps - 1)
        if states:

            def fetch(t):
                rows = pl.ds(pl.multiple_of(t * 256, 256), 256)
                return pltpu.make_async_copy(h_ref.at[rows, :], h_s.at[t % 2], h_sem.at[t % 2])

            def store(t):
                rows = pl.ds(pl.multiple_of(t * 256, 256), 256)
                return pltpu.make_async_copy(dh_s.at[t % 2], dh_ref.at[rows, :], dh_sem.at[t % 2])

            fetch(0).start()

            def back(t, _):
                r = pl.ds(pl.multiple_of(t * 256, 256), 256)
                fetch(t).wait()
                pl.when(t + 1 < n // 256)(lambda: fetch(t + 1).start())
                da = da_s[r, :].astype(BF).astype(F32)
                wide = h_s[t % 2].astype(F32)
                s = norm_scale(wide)
                dx = s * (da - wide * (s * s * jnp.mean(da * wide, -1, keepdims=True)))
                pl.when(t >= 2)(lambda: store(t - 2).wait())
                dh_s[t % 2] = (dy_ref[r, :].astype(F32) + dx.astype(BF).astype(F32)).astype(BF)
                store(t).start()
                return 0

            lax.fori_loop(0, n // 256, back, 0)
            store(n // 256 - 2).wait()
            store(n // 256 - 1).wait()
        pair_second(steps - 1)
        pair_last(steps - 2)
        pair_last(steps - 1)


def backward(number, a, dy, act, sa, sb, weights, h=None, tokens=512, tile=512):
    wg, wu, wd = weights
    n, d = a.shape
    ff = act.shape[1]
    parts, steps, states = n // tokens, ff // tile, h is not None
    column = lambda i: jnp.maximum(i - 4, 0) // parts
    part = lambda i: jnp.maximum(i - 4, 0) % parts
    saved = pl.BlockSpec((tokens, tile), lambda i: (part(i), column(i)))
    rows_of = pl.BlockSpec((None, tile, d), lambda i: (number, column(i), 0))
    columns_of = pl.BlockSpec((None, d, tile), lambda i: (number, 0, column(i)))
    dma = pltpu.SemaphoreType.DMA
    v = lambda *shape: pltpu.VMEM(shape, BF)
    f = lambda *shape: pltpu.VMEM(shape, F32)
    r, q = ff // 8, ff // 16
    down_scratch = [v(2, 2, r, d)] * 3 + [f(2, q, d)] * 2 + [v(2, q, d)] * 4 + [v(q, d)] * 4
    p = d // 8
    pair_scratch = [v(2, 2, p, tile)] * 2 + [v(2, 2, 2, p, tile), f(2, 2, p, tile)]
    pair_scratch += [v(2, p, tile), v(steps, 2, p, tile), v(2, p, tile), v(steps, p, tile)]
    sems = [dma((2, 4)), dma((2, 4)), dma((2, 2, 2)), dma((2, 4, steps))]
    return pl.pallas_call(
        functools.partial(backward_kernel, states, tokens, tile, steps),
        grid=(4 + steps * parts,),
        in_specs=[
            whole((n, d)),
            whole((n, d)),
            pl.BlockSpec((n, ff // 4), lambda i: (0, jnp.minimum(i, 3))),
            saved,
            saved,
            rows_of,
        ]
        + [pl.BlockSpec(memory_space=pl.ANY), columns_of, columns_of] * states,
        out_specs=[whole((p, ff)), whole((p, ff)), whole((r, d))] + [pl.BlockSpec(memory_space=pl.ANY)] * states,
        out_shape=[sds((p, ff), BF), sds((p, ff), BF), sds((r, d), BF)] + [sds((n, d), BF)] * states,
        scratch_shapes=[v(n, tile)] * 2 + down_scratch + pair_scratch * 2 + sems + [f(n, d), v(2, 256, d), v(2, 256, d), dma((2,)), dma((2,))] * states,
        compiler_params=pltpu.CompilerParams(
            vmem_limit_bytes=VMEM, collective_id=number, has_side_effects=True
        ),
        cost_estimate=cost(6 if states else 4, n, d, ff, 12 * n * ff),
        name="backward",
    )(a, dy, act, sa, sb, wd, *([h, wg, wu] if states else []))


def swap(value, bit):
    return lax.ppermute(value, "dp", [(i, i ^ bit) for i in range(8)])


def all_gather(mine):
    layers, rows, columns = mine.shape
    half = rows // 32 * 16
    me = lax.axis_index("dp")
    by_x, by_y = swap(mine, X), swap(mine, Y)
    far_a, far_b = swap(by_x[:, :half], Y), swap(by_y[:, half:], X)
    out = jnp.zeros((layers, 8 * rows, columns), mine.dtype)
    for bit, off, block in ((0, 0, mine), (X, 0, by_x), (Y, 0, by_y), (X ^ Y, 0, far_a), (X ^ Y, half, far_b)):
        for core, part in ((0, block), (CORE, swap(block, CORE))):
            out = lax.dynamic_update_slice(out, part, (0, (me ^ bit ^ core) * rows + off, 0))
    return out


def adamw(w, m, v, g):
    m = 0.9 * m + 0.1 * g
    v = 0.95 * v + 0.05 * g * g
    step = m * lax.rsqrt(v + 1e-8) + 0.1 * w
    return (w - 0.02 * step).astype(BF), m, v


def solution(mesh):
    def step(x, dy, *arrays):
        weights, ms, vs = (arrays[i : i + 3] for i in (0, 3, 6))
        h0, dy = x[0], dy[0]
        me = lax.axis_index("dp")
        a0, act0, sa0, sb0, h1 = forward(0, h0, weights, True)
        a1, act1, sa1, sb1 = forward(1, h1, weights, False)
        gate1, up1, down1, dh1 = backward(1, a1, dy, act1, sa1, sb1, weights, h1)
        gate0, up0, down0 = backward(0, a0, dh1, act0, sa0, sb0, weights, tokens=1024)

        gradients = [jnp.stack(t).astype(F32) for t in ((gate0, gate1), (up0, up1), (down0, down1))]
        squares = sum(jnp.sum(g * g) for g in gradients).reshape(1, 1)
        for bit in (CORE, Y, X):
            squares = squares + swap(squares, bit)
        count = sum(w.size for w in weights)
        factor = jnp.minimum(1.0, 0.5 * lax.rsqrt(squares[0, 0] / count + 1e-30))
        new = []
        for w, m, v, g in zip(weights, ms, vs, gradients, strict=True):
            mine = lax.dynamic_slice_in_dim(w, me * m.shape[1], m.shape[1], axis=1)
            new.append(adamw(mine.astype(F32), m, v, g * factor))
        return tuple(all_gather(w) for w, _, _ in new) + tuple(m for _, m, _ in new) + tuple(v for _, _, v in new)

    batch, rows = P(("rep", "dp")), P(None, "dp")
    return jax.shard_map(
        step,
        mesh=mesh,
        in_specs=(batch,) * 2 + (P(),) * 3 + (rows,) * 6,
        out_specs=(P("rep"),) * 3 + (P("rep", "dp"),) * 6,
        check_vma=False,
    )
```

```python
import functools

import jax
import jax.numpy as jnp
from jax import lax
from jax.experimental import pallas as pl
from jax.experimental.pallas import tpu as pltpu
from jax.sharding import PartitionSpec as P


F32, BF = jnp.float32, jnp.bfloat16
VMEM = 67043328
X, Y, CORE = 4, 2, 1
PARTS = 2


def dot(a, b, ca=1, cb=0):
    return lax.dot_general(a, b, (((ca,), (cb,)), ((), ())), preferred_element_type=F32)


def norm_scale(wide):
    return lax.rsqrt(jnp.mean(wide * wide, -1, keepdims=True) + 1e-6)


def whole(shape):
    return pl.BlockSpec(shape, lambda i, *_: (0,) * len(shape), pipeline_mode=pl.Buffered(1))


def sds(shape, dtype):
    return jax.ShapeDtypeStruct(shape, dtype)


def params():
    return pltpu.CompilerParams(vmem_limit_bytes=VMEM)


def cost(matmuls, n, d, ff, bytes_accessed):
    return pl.CostEstimate(flops=2 * matmuls * n * d * ff, bytes_accessed=bytes_accessed, transcendentals=0)


def forward_kernel(chunk, down, h_ref, wg_ref, wu_ref, *refs):
    if down:
        wd_ref, a_ref, act_ref, sa_ref, sb_ref, h1_ref = refs
    else:
        a_ref, act_ref, sa_ref, sb_ref = refs
    wide = h_ref[...].astype(F32)
    a = (wide * norm_scale(wide)).astype(BF)
    a_ref[...] = a
    for c in range(wg_ref.shape[1] // chunk):
        s = pl.ds(c * chunk, chunk)
        gate, up = dot(a, wg_ref[:, s]), dot(a, wu_ref[:, s])
        sig = 1.0 / (1.0 + jnp.exp(-gate))
        silu = gate * sig
        act_ref[:, s] = (silu * up).astype(BF)
        sb_ref[:, s] = silu
        sa_ref[:, s] = up * (sig + silu * (1.0 - sig))
    if down:
        out = dot(act_ref[...], wd_ref[...]).astype(BF)
        h1_ref[...] = (h_ref[...].astype(F32) + out.astype(F32)).astype(BF)


def forward(number, h, weights, down, tile=256, chunk=1280):
    n, d = h.shape
    ff = weights[0].shape[2]
    row = lambda w: pl.BlockSpec((tile, w), lambda i: (i, 0))
    of = lambda w: pl.BlockSpec((None, *w.shape[1:]), lambda i: (number, 0, 0), pipeline_mode=pl.Buffered(1))
    used = weights[: 2 + down]
    return pl.pallas_call(
        functools.partial(forward_kernel, chunk, down),
        grid=(n // tile,),
        in_specs=[row(d)] + [of(w) for w in used],
        out_specs=[row(d), row(ff), row(ff), row(ff)] + [row(d)] * down,
        out_shape=[sds((n, d), BF), sds((n, ff), BF), sds((n, ff), F32), sds((n, ff), F32)] + [sds((n, d), BF)] * down,
        compiler_params=params(),
        cost_estimate=cost(3 if down else 2, n, d, ff, 10 * n * ff),
        name="forward",
    )(h, *used)


def peers():
    me = lax.axis_index("dp")
    x, y, core = me // 4, me // 2 % 2, me % 2
    return (x, y, core), (me + 1 - 2 * core, me + 2 - 4 * y, me + 4 - 8 * x)


def xor(a, b):
    return a + b - 2 * a * b


def send(src, dst, sems, to):
    return pltpu.make_async_remote_copy(
        src_ref=src,
        dst_ref=dst,
        send_sem=sems[0],
        recv_sem=sems[1],
        device_id={"dp": to},
        device_id_type=pl.DeviceIdType.MESH,
    )


def total(*terms):
    return sum(t.astype(F32) for t in terms)


def backward_kernel(states, tokens, tile, steps, *refs):
    refs = list(refs)
    take = lambda k: [refs.pop(0) for _ in range(k)]
    a_ref, dy_ref, act_ref, sa_ref, sb_ref, wd_ref = take(6)
    h_ref, wg_ref, wu_ref = take(3) if states else (None,) * 3
    (before_ref,) = (None,) if states else take(1)
    gate_ref, up_ref, down_ref = take(3)
    (squares_ref,) = take(1)
    (dh_ref,) = take(1) if states else (None,)
    dg_s, du_s = take(2)
    dk, do, di, da_sum, db_sum, dsx, dsy, drx, dry, dsy2, dsx2, dry2, drx2 = take(13)
    gk, go, gi, g_sum, gs1, gr1, gs2, gr2 = take(8)
    uk, uo, ui, u_sum, us1, ur1, us2, ur2 = take(8)
    d_core, d_link, p_core, p_link = take(4)
    if states:
        da_s, h_s, dh_s, h_sem, dh_sem = take(5)
    else:
        sq_s, sq_in, sq_sem = take(3)

    n, d = a_ref.shape
    parts = n // tokens
    i = pl.program_id(0)
    (x, y, core), (to_core, to_y, to_x) = peers()
    mine = core == 0

    def down_copy(q):
        sx, sy = xor(q // 2, x), xor(q % 2, y)
        return send(do.at[sx, sy], di.at[sx, sy], (d_core.at[0, q], d_core.at[1, q]), to_core)

    def down_links(stage):
        sem = lambda k: (d_link.at[0, k], d_link.at[1, k])
        if stage == 1:
            return send(dsx, drx, sem(0), to_x), send(dsy, dry, sem(1), to_y)
        return send(dsy2, dry2, sem(2), to_y), send(dsx2, drx2, sem(3), to_x)

    def core_copy(which, u):
        src, dst = ((go, gi), (uo, ui))[which]
        slot = u % 2
        return send(src, dst.at[slot], (p_core.at[0, which, slot], p_core.at[1, which, slot]), to_core)

    def pair_links(stage, u):
        sem = lambda k: (p_link.at[0, k, u], p_link.at[1, k, u])
        if stage == 1:
            return send(gs1, gr1.at[u], sem(0), to_x), send(us1, ur1.at[u], sem(1), to_y)
        return send(gs2.at[u % 2], gr2.at[u], sem(2), to_y), send(us2.at[u % 2], ur2.at[u], sem(3), to_x)

    def start(copies):
        for c in copies:
            c.start()

    def wait(copies):
        for c in copies:
            c.wait()

    def other(k):
        return 4 * xor(x, k // 4) + 2 * xor(y, k // 2 % 2) + xor(core, k % 2)

    def square_sum():
        return sum(jnp.sum(jnp.square(ref[...].astype(F32))) for ref in (gate_ref, up_ref, down_ref))

    half = dk.shape[2] // 2
    lo, hi = pl.ds(0, half), pl.ds(half, half)

    def down_first():
        wait([down_copy(q) for q in range(4)])
        dsx[...] = total(dk[1, :, lo], di[1, :, lo]).astype(BF)
        dsy[...] = total(dk[:, 1, hi], di[:, 1, hi]).astype(BF)
        start(down_links(1))
        da_sum[...] = total(dk[0, :, lo], di[0, :, lo])
        db_sum[...] = total(dk[:, 0, hi], di[:, 0, hi])

    def down_second():
        wait(down_links(1))
        dsy2[...] = total(da_sum[1], drx[1]).astype(BF)
        dsx2[...] = total(db_sum[1], dry[1]).astype(BF)
        start(down_links(2))
        da_sum[0] = total(da_sum[0], drx[0])
        db_sum[0] = total(db_sum[0], dry[0])

    def down_last():
        wait(down_links(2))
        down_ref[lo, :] = total(da_sum[0], dry2[...]).astype(BF)
        down_ref[hi, :] = total(db_sum[0], drx2[...]).astype(BF)

    def pair_first(u):
        slot = u % 2
        wait([core_copy(0, u), core_copy(1, u)])
        gs1[...] = total(gk[1], gi[slot, 1]).astype(BF)
        us1[...] = total(uk[:, 1], ui[slot, :, 1]).astype(BF)
        start(pair_links(1, u))
        g_sum[slot] = total(gk[0], gi[slot, 0])
        u_sum[slot] = total(uk[:, 0], ui[slot, :, 0])

    def pair_second(u):
        slot = u % 2
        wait(pair_links(1, u))
        gs2[slot] = total(g_sum[slot, 1], gr1[u, 1]).astype(BF)
        us2[slot] = total(u_sum[slot, 1], ur1[u, 1]).astype(BF)
        start(pair_links(2, u))
        g_sum[slot, 0] = total(g_sum[slot, 0], gr1[u, 0])
        u_sum[slot, 0] = total(u_sum[slot, 0], ur1[u, 0])

    def pair_last(u):
        slot = u % 2
        wait(pair_links(2, u))
        cols = pl.ds(pl.multiple_of(u * tile, tile), tile)
        gate_ref[:, cols] = total(g_sum[slot, 0], gr2[u]).astype(BF)
        up_ref[:, cols] = total(u_sum[slot, 0], ur2[u]).astype(BF)

    @pl.when(i == 0)
    def _():
        barrier = pltpu.get_barrier_semaphore()
        met = (to_core, to_y, to_x) if states else [other(k) for k in range(1, 8)]
        for to in met:
            pl.semaphore_signal(barrier, inc=1, device_id={"dp": to}, device_id_type=pl.DeviceIdType.MESH)
        pl.semaphore_wait(barrier, len(met))
        if states:

            def clear(t, _):
                da_s[pl.ds(pl.multiple_of(t * 256, 256), 256), :] = jnp.zeros((256, d), F32)
                return 0

            lax.fori_loop(0, n // 256, clear, 0)

    @pl.when(i < 4)
    def _():
        g = dot(act_ref[...], dy_ref[...], 0, 0)
        rows = g.shape[0] // 2
        sx, sy = xor(i // 2, x), xor(i % 2, y)
        dk[sx, sy] = jnp.where(mine, g[:rows], g[rows:]).astype(BF)
        do[sx, sy] = jnp.where(mine, g[rows:], g[:rows]).astype(BF)
        down_copy(i).start()

    @pl.when(i >= 4)
    def _():
        j, t = (i - 4) // parts, (i - 4) % parts
        r = pl.ds(pl.multiple_of(t * tokens, tokens), tokens)
        dp = dot(dy_ref[r, :], wd_ref[...], 1, 1).astype(BF).astype(F32)
        du = (dp * sb_ref[...]).astype(BF)
        dg = (dp * sa_ref[...]).astype(BF)
        dg_s[r, :], du_s[r, :] = dg, du
        if states:
            da_s[r, :] += dot(dg, wg_ref[...], 1, 1) + dot(du, wu_ref[...], 1, 1)

        @pl.when(t == parts - 1)
        def _():
            pl.when(j == 0)(down_first)
            pl.when(j == 2)(down_second)
            pl.when(j >= 2)(lambda: pair_second(j - 2))
            pl.when(j >= 3)(lambda: pair_last(j - 3))
            pl.when(j >= 1)(lambda: pair_first(j - 1))
            pl.when(j == 3)(down_last)
            rows = d // 8
            for which, (by, keep, out) in enumerate(((dg_s, gk, go), (du_s, uk, uo))):
                g = dot(a_ref[...], by[...], 0, 0)
                for q in range(4):
                    first, second = (g[(2 * q + e) * rows : (2 * q + e + 1) * rows] for e in (0, 1))
                    sx, sy = xor(q // 2, x), xor(q % 2, y)
                    keep[sx, sy] = jnp.where(mine, first, second).astype(BF)
                    out[sx, sy] = jnp.where(mine, second, first).astype(BF)
                core_copy(which, j).start()

    @pl.when(i == 4 + steps * parts - 1)
    def _():
        pair_second(steps - 2)
        pair_last(steps - 3)
        pair_first(steps - 1)
        if states:

            def fetch(t):
                rows = pl.ds(pl.multiple_of(t * 256, 256), 256)
                return pltpu.make_async_copy(h_ref.at[rows, :], h_s.at[t % 2], h_sem.at[t % 2])

            def store(t):
                rows = pl.ds(pl.multiple_of(t * 256, 256), 256)
                return pltpu.make_async_copy(dh_s.at[t % 2], dh_ref.at[rows, :], dh_sem.at[t % 2])

            fetch(0).start()

            def back(t, _):
                r = pl.ds(pl.multiple_of(t * 256, 256), 256)
                fetch(t).wait()
                pl.when(t + 1 < n // 256)(lambda: fetch(t + 1).start())
                da = da_s[r, :].astype(BF).astype(F32)
                wide = h_s[t % 2].astype(F32)
                s = norm_scale(wide)
                dx = s * (da - wide * (s * s * jnp.mean(da * wide, -1, keepdims=True)))
                pl.when(t >= 2)(lambda: store(t - 2).wait())
                dh_s[t % 2] = (dy_ref[r, :].astype(F32) + dx.astype(BF).astype(F32)).astype(BF)
                store(t).start()
                return 0

            lax.fori_loop(0, n // 256, back, 0)
            store(n // 256 - 2).wait()
            store(n // 256 - 1).wait()
        pair_second(steps - 1)
        pair_last(steps - 2)
        pair_last(steps - 1)
        if states:
            squares_ref[...] = jnp.full(squares_ref.shape, square_sum(), F32)
            return
        sq_s[...] = before_ref[...] + square_sum()
        copies = [send(sq_s, sq_in.at[k], (sq_sem.at[0, k], sq_sem.at[1, k]), other(k)) for k in range(1, 8)]
        start(copies)
        wait(copies)
        sq_in[0] = sq_s[...]
        parts_of = [sq_in[k] for k in range(8)]
        while len(parts_of) > 1:
            parts_of = [one + two for one, two in zip(parts_of[::2], parts_of[1::2], strict=True)]
        squares_ref[...] = parts_of[0]


def backward(number, a, dy, act, sa, sb, weights, h=None, before=None, tokens=512, tile=512):
    wg, wu, wd = weights
    n, d = a.shape
    ff = act.shape[1]
    parts, steps, states = n // tokens, ff // tile, h is not None
    column = lambda i: jnp.maximum(i - 4, 0) // parts
    part = lambda i: jnp.maximum(i - 4, 0) % parts
    saved = pl.BlockSpec((tokens, tile), lambda i: (part(i), column(i)))
    rows_of = pl.BlockSpec((None, tile, d), lambda i: (number, column(i), 0))
    columns_of = pl.BlockSpec((None, d, tile), lambda i: (number, 0, column(i)))
    dma = pltpu.SemaphoreType.DMA
    v = lambda *shape: pltpu.VMEM(shape, BF)
    f = lambda *shape: pltpu.VMEM(shape, F32)
    r, q = ff // 8, ff // 16
    down_scratch = [v(2, 2, r, d)] * 3 + [f(2, q, d)] * 2 + [v(2, q, d)] * 4 + [v(q, d)] * 4
    p = d // 8
    pair_scratch = [v(2, 2, p, tile)] * 2 + [v(2, 2, 2, p, tile), f(2, 2, p, tile)]
    pair_scratch += [v(2, p, tile), v(steps, 2, p, tile), v(2, p, tile), v(steps, p, tile)]
    sems = [dma((2, 4)), dma((2, 4)), dma((2, 2, 2)), dma((2, 4, steps))]
    return pl.pallas_call(
        functools.partial(backward_kernel, states, tokens, tile, steps),
        grid=(4 + steps * parts,),
        in_specs=[
            whole((n, d)),
            whole((n, d)),
            pl.BlockSpec((n, ff // 4), lambda i: (0, jnp.minimum(i, 3))),
            saved,
            saved,
            rows_of,
        ]
        + ([pl.BlockSpec(memory_space=pl.ANY), columns_of, columns_of] if states else [whole((8, 128))]),
        out_specs=[whole((p, ff)), whole((p, ff)), whole((r, d)), whole((8, 128))] + [pl.BlockSpec(memory_space=pl.ANY)] * states,
        out_shape=[sds((p, ff), BF), sds((p, ff), BF), sds((r, d), BF), sds((8, 128), F32)]
        + [sds((n, d), BF)] * states,
        scratch_shapes=[v(n, tile)] * 2 + down_scratch + pair_scratch * 2 + sems
        + ([f(n, d), v(2, 256, d), v(2, 256, d), dma((2,)), dma((2,))] if states else [f(8, 128), f(8, 8, 128), dma((2, 8))]),
        compiler_params=pltpu.CompilerParams(
            vmem_limit_bytes=VMEM, collective_id=number, has_side_effects=True
        ),
        cost_estimate=cost(6 if states else 4, n, d, ff, 12 * n * ff),
        name="backward",
    )(a, dy, act, sa, sb, wd, *([h, wg, wu] if states else [before]))


def swap(value, bit):
    return lax.ppermute(value, "dp", [(i, i ^ bit) for i in range(8)])


def adamw_kernel(count, me_ref, squares_ref, g0_ref, g1_ref, w_ref, m_ref, v_ref, wo_ref, mo_ref, vo_ref):
    factor = jnp.minimum(1.0, 0.5 * lax.rsqrt(squares_ref[0:1, 0:1] / count + 1e-30))
    g = jnp.where(pl.program_id(0) == 0, g0_ref[...].astype(F32), g1_ref[...].astype(F32)) * factor
    m = 0.9 * m_ref[...] + 0.1 * g
    v = 0.95 * v_ref[...] + 0.05 * g * g
    step = m * lax.rsqrt(v + 1e-8) + 0.1 * w_ref[...].astype(F32)
    wo_ref[...] = (w_ref[...].astype(F32) - 0.02 * step).astype(BF)
    mo_ref[...], vo_ref[...] = m, v


def adamw(me, squares, count, g0, g1, w, m, v):
    _, rows, columns = m.shape
    by_columns = rows < 128
    block = (rows, columns // PARTS) if by_columns else (rows // PARTS, columns)
    at = (lambda c: (0, c)) if by_columns else (lambda c: (c, 0))
    grad = pl.BlockSpec(block, lambda l, c, s: at(c))
    state = pl.BlockSpec((None, *block), lambda l, c, s: (l, *at(c)))
    mine = (lambda l, c, s: (l, s[0], c)) if by_columns else (lambda l, c, s: (l, s[0] * PARTS + c, 0))
    return pl.pallas_call(
        functools.partial(adamw_kernel, count),
        grid_spec=pltpu.PrefetchScalarGridSpec(
            num_scalar_prefetch=1,
            grid=(2, PARTS),
            in_specs=[whole((8, 128)), grad, grad, pl.BlockSpec((None, *block), mine), state, state],
            out_specs=[state] * 3,
        ),
        out_shape=[sds(m.shape, BF), sds(m.shape, F32), sds(m.shape, F32)],
        compiler_params=params(),
        cost_estimate=pl.CostEstimate(flops=m.size * 4000, bytes_accessed=m.size * 22, transcendentals=0),
        name="adamw",
    )(me, squares, g0, g1, w, m, v)


def place_kernel(pieces, *refs):
    refs = list(refs)
    blocks, out = refs[: len(pieces)], refs[-3]
    buffer, sems = refs[-2], refs[-1]
    (x, y, core), _ = peers()
    todo = []
    at = 0
    for (bit, off), block in zip(pieces, blocks, strict=True):
        rows = block.shape[1]
        slot = 4 * xor(x, bit // 4) + 2 * xor(y, bit // 2 % 2) + xor(core, bit % 2)
        for number in range(block.shape[0]):
            k = len(todo)
            held = buffer.at[pl.ds(at, rows)]
            at += rows
            todo.append(
                (
                    pltpu.make_async_copy(block.at[number], held, sems.at[0, k]),
                    pltpu.make_async_copy(held, out.at[number, slot, pl.ds(off, rows)], sems.at[1, k]),
                )
            )
    for fetch, _ in todo:
        fetch.start()
    for fetch, store in todo:
        fetch.wait()
        store.start()
    for _, store in todo:
        store.wait()


def place(pieces, blocks, into=None, shape=None):
    layers, columns = blocks[0].shape[0], blocks[0].shape[2]
    anywhere = pl.BlockSpec(memory_space=pl.ANY)
    total_rows = layers * sum(b.shape[1] for b in blocks)
    size = 4 * total_rows * columns
    return pl.pallas_call(
        functools.partial(place_kernel, pieces),
        in_specs=[anywhere] * (len(blocks) + (into is not None)),
        out_specs=anywhere,
        out_shape=sds(shape, BF),
        scratch_shapes=[pltpu.VMEM((total_rows, columns), BF), pltpu.SemaphoreType.DMA((2, layers * len(blocks)))],
        input_output_aliases={len(blocks): 0} if into is not None else {},
        compiler_params=params(),
        cost_estimate=pl.CostEstimate(flops=size * 300, bytes_accessed=size, transcendentals=0),
        name="place",
    )(*blocks, *([into] if into is not None else []))


def all_gather(mine):
    done = []
    for w in mine:
        half = w.shape[1] // 32 * 16
        bx, by, bc = (swap(w, bit) for bit in (X, Y, CORE))
        fa = swap(bx[:, :half], Y)
        fb = swap(by[:, half:], X)
        cx, cy = (swap(t, CORE) for t in (bx, by))
        shape = (w.shape[0], 8, *w.shape[1:])
        near = ((0, 0), (1, 0), (4, 0), (5, 0), (2, 0), (3, 0))
        out = place(near, (w, bc, bx, cx, by, cy), None, shape)
        ca, cb = (swap(t, CORE) for t in (fa, fb))
        rest = ((6, 0), (7, 0), (6, half), (7, half))
        out = place(rest, (fa, ca, fb, cb), out, shape)
        done.append(out.reshape(w.shape[0], -1, w.shape[2]))
    return done


def solution(mesh):
    def step(x, dy, *arrays):
        weights, ms, vs = (arrays[i : i + 3] for i in (0, 3, 6))
        h0, dy = x[0], dy[0]
        me = lax.axis_index("dp").astype(jnp.int32).reshape(1)
        a0, act0, sa0, sb0, h1 = forward(0, h0, weights, True)
        a1, act1, sa1, sb1 = forward(1, h1, weights, False)
        *second, squares, dh1 = backward(1, a1, dy, act1, sa1, sb1, weights, h1)
        *first, squares = backward(0, a0, dh1, act0, sa0, sb0, weights, before=squares, tokens=1024)
        count = sum(w.size for w in weights)
        new = [adamw(me, squares, count, *args) for args in zip(first, second, weights, ms, vs, strict=True)]
        whole_weights = all_gather([w for w, _, _ in new])
        return (*whole_weights, *(m for _, m, _ in new), *(v for _, _, v in new))

    batch, rows = P(("rep", "dp")), P(None, "dp")
    return jax.shard_map(
        step,
        mesh=mesh,
        in_specs=(batch,) * 2 + (P(),) * 3 + (rows,) * 6,
        out_specs=(P("rep"),) * 3 + (P("rep", "dp"),) * 6,
        check_vma=False,
    )
```

```python
import functools

import jax
import jax.numpy as jnp
from jax import lax
from jax.experimental import pallas as pl
from jax.experimental.pallas import tpu as pltpu
from jax.sharding import PartitionSpec as P


F32, BF = jnp.float32, jnp.bfloat16
VMEM = 67043328
X, Y, CORE = 4, 2, 1
PARTS = 2


def dot(a, b, ca=1, cb=0):
    return lax.dot_general(a, b, (((ca,), (cb,)), ((), ())), preferred_element_type=F32)


def norm_scale(wide):
    return lax.rsqrt(jnp.mean(wide * wide, -1, keepdims=True) + 1e-6)


def whole(shape):
    return pl.BlockSpec(shape, lambda i, *_: (0,) * len(shape), pipeline_mode=pl.Buffered(1))


def sds(shape, dtype):
    return jax.ShapeDtypeStruct(shape, dtype)


def params():
    return pltpu.CompilerParams(vmem_limit_bytes=VMEM)


def cost(matmuls, n, d, ff, bytes_accessed):
    return pl.CostEstimate(flops=2 * matmuls * n * d * ff, bytes_accessed=bytes_accessed, transcendentals=0)


def forward_kernel(chunk, down, h_ref, wg_ref, wu_ref, *refs):
    if down:
        wd_ref, a_ref, act_ref, sa_ref, sb_ref, h1_ref = refs
    else:
        a_ref, act_ref, sa_ref, sb_ref = refs
    wide = h_ref[...].astype(F32)
    a = (wide * norm_scale(wide)).astype(BF)
    a_ref[...] = a
    for c in range(wg_ref.shape[1] // chunk):
        s = pl.ds(c * chunk, chunk)
        gate, up = dot(a, wg_ref[:, s]), dot(a, wu_ref[:, s])
        sig = 1.0 / (1.0 + jnp.exp(-gate))
        silu = gate * sig
        act_ref[:, s] = (silu * up).astype(BF)
        sb_ref[:, s] = silu
        sa_ref[:, s] = up * (sig + silu * (1.0 - sig))
    if down:
        out = dot(act_ref[...], wd_ref[...]).astype(BF)
        h1_ref[...] = (h_ref[...].astype(F32) + out.astype(F32)).astype(BF)


def forward(number, h, weights, down, tile=256, chunk=1280):
    n, d = h.shape
    ff = weights[0].shape[2]
    row = lambda w: pl.BlockSpec((tile, w), lambda i: (i, 0))
    of = lambda w: pl.BlockSpec((None, *w.shape[1:]), lambda i: (number, 0, 0), pipeline_mode=pl.Buffered(1))
    used = weights[: 2 + down]
    return pl.pallas_call(
        functools.partial(forward_kernel, chunk, down),
        grid=(n // tile,),
        in_specs=[row(d)] + [of(w) for w in used],
        out_specs=[row(d), row(ff), row(ff), row(ff)] + [row(d)] * down,
        out_shape=[sds((n, d), BF), sds((n, ff), BF), sds((n, ff), F32), sds((n, ff), F32)] + [sds((n, d), BF)] * down,
        compiler_params=params(),
        cost_estimate=cost(3 if down else 2, n, d, ff, 10 * n * ff),
        name="forward",
    )(h, *used)


def peers():
    me = lax.axis_index("dp")
    x, y, core = me // 4, me // 2 % 2, me % 2
    return (x, y, core), (me + 1 - 2 * core, me + 2 - 4 * y, me + 4 - 8 * x)


def xor(a, b):
    return a + b - 2 * a * b


def send(src, dst, sems, to):
    return pltpu.make_async_remote_copy(
        src_ref=src,
        dst_ref=dst,
        send_sem=sems[0],
        recv_sem=sems[1],
        device_id={"dp": to},
        device_id_type=pl.DeviceIdType.MESH,
    )


def total(*terms):
    return sum(t.astype(F32) for t in terms)


def backward_kernel(states, tokens, tile, steps, *refs):
    refs = list(refs)
    take = lambda k: [refs.pop(0) for _ in range(k)]
    a_ref, dy_ref, act_ref, sa_ref, sb_ref, wd_ref = take(6)
    if states:
        h_ref, wg_ref, wu_ref = take(3)
    else:
        before_ref, left_ref, gate1_ref, up1_ref = take(4)
    gate_ref, up_ref, down_ref, squares_ref = take(4)
    if states:
        dh_ref, left_ref = take(2)
    else:
        gate1_out, up1_out = take(2)
    dg_s, du_s, act_s, act_sem = take(4)
    dk, do, di, da_sum, db_sum, dsx, dsy, drx, dry, dsy2, dsx2, dry2, drx2 = take(13)
    gk, go, gi, g_sum, gs1, gr1, gs2, gr2 = take(8)
    uk, uo, ui, u_sum, us1, ur1, us2, ur2 = take(8)
    d_core, d_link, p_core, p_link, left_sem = take(5)
    if states:
        da_s, h_s, dh_s, h_sem, dh_sem = take(5)
    else:
        sq_s, sq_in, sq_sem = take(3)

    n, d = a_ref.shape
    parts = n // tokens
    i = pl.program_id(0)
    (x, y, core), (to_core, to_y, to_x) = peers()
    mine = core == 0

    def other(k):
        return 4 * xor(x, k // 4) + 2 * xor(y, k // 2 % 2) + xor(core, k % 2)

    def start(copies):
        for c in copies:
            c.start()

    def wait(copies):
        for c in copies:
            c.wait()

    def down_copy(k):
        slot = 1 - k // 2, 1 - k % 2
        return send(do.at[slot], di.at[slot], (d_core.at[0, k], d_core.at[1, k]), to_core)

    def fetch_act(k):
        width = act_s.shape[2]
        q = 2 * xor(1 - k // 2, x) + xor(1 - k % 2, y)
        columns = pl.ds(pl.multiple_of(q * width, 128), width)
        return pltpu.make_async_copy(act_ref.at[:, columns], act_s.at[k % 2], act_sem.at[k % 2])

    def down_links(stage, way):
        sem = lambda k: (d_link.at[0, k], d_link.at[1, k])
        if stage == 1:
            return send(dsx, drx, sem(0), to_x) if way == "x" else send(dsy, dry, sem(1), to_y)
        return send(dsx2, drx2, sem(3), to_x) if way == "x" else send(dsy2, dry2, sem(2), to_y)

    def core_copy(which, u):
        src, dst = ((go, gi), (uo, ui))[which]
        slot = u % 2
        return send(src, dst.at[slot], (p_core.at[0, which, slot], p_core.at[1, which, slot]), to_core)

    def pair_links(stage, u):
        sem = lambda k: (p_link.at[0, k, u], p_link.at[1, k, u])
        slot = u % 2
        if stage == 1:
            return send(gs1.at[slot], gr1.at[u], sem(0), to_x), send(us1.at[slot], ur1.at[u], sem(1), to_y)
        return send(gs2.at[slot], gr2.at[u], sem(2), to_y), send(us2.at[slot], ur2.at[u], sem(3), to_x)

    half = dk.shape[2] // 2
    lo, hi = pl.ds(0, half), pl.ds(half, half)

    def down_x():
        wait([down_copy(0), down_copy(1)])
        dsx[...] = total(dk[1, :, lo], di[1, :, lo]).astype(BF)
        down_links(1, "x").start()

    def down_y():
        wait([down_copy(2)])
        dsy[...] = total(dk[:, 1, hi], di[:, 1, hi]).astype(BF)
        down_links(1, "y").start()

    def down_sums():
        wait([down_copy(3)])
        da_sum[...] = total(dk[0, :, lo], di[0, :, lo])
        db_sum[...] = total(dk[:, 0, hi], di[:, 0, hi])

    def down_second():
        down_links(1, "x").wait()
        dsy2[...] = total(da_sum[1], drx[1]).astype(BF)
        down_links(2, "y").start()
        da_sum[0] = total(da_sum[0], drx[0])
        down_links(1, "y").wait()
        dsx2[...] = total(db_sum[1], dry[1]).astype(BF)
        down_links(2, "x").start()
        db_sum[0] = total(db_sum[0], dry[0])

    def down_last():
        down_links(2, "y").wait()
        down_links(2, "x").wait()
        down_ref[lo, :] = total(da_sum[0], dry2[...]).astype(BF)
        down_ref[hi, :] = total(db_sum[0], drx2[...]).astype(BF)

    def pair_first(u):
        slot, held = u % 2, u % 3
        wait([core_copy(0, u), core_copy(1, u)])
        gs1[slot] = total(gk[1], gi[slot, 1]).astype(BF)
        us1[slot] = total(uk[:, 1], ui[slot, :, 1]).astype(BF)
        start(pair_links(1, u))
        g_sum[held] = total(gk[0], gi[slot, 0])
        u_sum[held] = total(uk[:, 0], ui[slot, :, 0])

    def pair_second(u):
        slot, held = u % 2, u % 3
        wait(pair_links(1, u))
        gs2[slot] = total(g_sum[held, 1], gr1[u, 1]).astype(BF)
        us2[slot] = total(u_sum[held, 1], ur1[u, 1]).astype(BF)
        start(pair_links(2, u))
        g_sum[held, 0] = total(g_sum[held, 0], gr1[u, 0])
        u_sum[held, 0] = total(u_sum[held, 0], ur1[u, 0])

    def pair_last(u, gate_to=None, up_to=None, column=None):
        held = u % 3
        wait(pair_links(2, u))
        column = u if column is None else column
        cols = pl.ds(pl.multiple_of(column * tile, tile), tile)
        gate_to, up_to = (gate_ref, up_ref) if gate_to is None else (gate_to, up_to)
        gate_to[:, cols] = total(g_sum[held, 0], gr2[u]).astype(BF)
        up_to[:, cols] = total(u_sum[held, 0], ur2[u]).astype(BF)

    def left_copies(fill):
        held = (gk, go, uk, uo)
        ends = [(left_ref.at[k], t) if fill else (t, left_ref.at[k]) for k, t in enumerate(held)]
        return [pltpu.make_async_copy(src, dst, left_sem.at[k]) for k, (src, dst) in enumerate(ends)]

    def squares_of(*values):
        return sum(jnp.sum(jnp.square(value.astype(F32))) for value in values)

    given = steps
    most = (steps - 1) * tile

    @pl.when(i == 0)
    def _():
        fetch_act(0).start()
        fetch_act(1).start()
        if not states:
            start(left_copies(True))
        barrier = pltpu.get_barrier_semaphore()
        met = (to_core, to_y, to_x) if states else [other(k) for k in range(1, 8)]
        for to in met:
            pl.semaphore_signal(barrier, inc=1, device_id={"dp": to}, device_id_type=pl.DeviceIdType.MESH)
        pl.semaphore_wait(barrier, len(met))
        if states:

            def clear(t, _):
                da_s[pl.ds(pl.multiple_of(t * 256, 256), 256), :] = jnp.zeros((256, d), F32)
                return 0

            lax.fori_loop(0, n // 256, clear, 0)
        else:
            wait(left_copies(True))
            core_copy(0, given).start()
            core_copy(1, given).start()
            gate1_out[:, :most] = gate1_ref[:, :most]
            up1_out[:, :most] = up1_ref[:, :most]

    @pl.when(i < 4)
    def _():
        fetch_act(i).wait()
        g = dot(act_s[i % 2], dy_ref[...], 0, 0)
        rows = g.shape[0] // 2
        sx, sy = 1 - i // 2, 1 - i % 2
        dk[sx, sy] = jnp.where(mine, g[:rows], g[rows:]).astype(BF)
        do[sx, sy] = jnp.where(mine, g[rows:], g[:rows]).astype(BF)
        down_copy(i).start()
        pl.when(i < 2)(lambda: fetch_act(i + 2).start())
        if not states:
            pl.when(i == 1)(lambda: pair_first(given))
            pl.when(i == 3)(lambda: pair_second(given))
        pl.when(i == 2)(down_x)
        pl.when(i == 3)(down_y)

    @pl.when(i >= 4)
    def _():
        j, t = (i - 4) // parts, (i - 4) % parts
        r = pl.ds(pl.multiple_of(t * tokens, tokens), tokens)
        dp = dot(dy_ref[r, :], wd_ref[...], 1, 1).astype(BF).astype(F32)
        du = (dp * sb_ref[...]).astype(BF)
        dg = (dp * sa_ref[...]).astype(BF)
        dg_s[r, :], du_s[r, :] = dg, du
        if states:
            da_s[r, :] += dot(dg, wg_ref[...], 1, 1) + dot(du, wu_ref[...], 1, 1)

        @pl.when(t == parts - 1)
        def _():
            pl.when(j == 0)(down_sums)
            pl.when(j >= 1)(lambda: pair_first(j - 1))
            pl.when(j == 1)(down_second)
            pl.when(j >= 2)(lambda: pair_second(j - 2))
            if not states:
                pl.when(j == 1)(lambda: pair_last(given, gate1_out, up1_out, steps - 1))
            pl.when(j == 2)(down_last)
            pl.when(j >= 3)(lambda: pair_last(j - 3))
            rows = d // 8
            for which, (by, keep, out) in enumerate(((dg_s, gk, go), (du_s, uk, uo))):
                g = dot(a_ref[...], by[...], 0, 0)
                for q in range(4):
                    first, second = (g[(2 * q + e) * rows : (2 * q + e + 1) * rows] for e in (0, 1))
                    sx, sy = xor(q // 2, x), xor(q % 2, y)
                    keep[sx, sy] = jnp.where(mine, first, second).astype(BF)
                    out[sx, sy] = jnp.where(mine, second, first).astype(BF)
                if states:
                    pl.when(j < steps - 1)(lambda: core_copy(which, j).start())
                else:
                    core_copy(which, j).start()

    @pl.when(i == 4 + steps * parts - 1)
    def _():
        if states:
            start(left_copies(False))
            pair_second(steps - 2)

            def fetch(t):
                rows = pl.ds(pl.multiple_of(t * 256, 256), 256)
                return pltpu.make_async_copy(h_ref.at[rows, :], h_s.at[t % 2], h_sem.at[t % 2])

            def store(t):
                rows = pl.ds(pl.multiple_of(t * 256, 256), 256)
                return pltpu.make_async_copy(dh_s.at[t % 2], dh_ref.at[rows, :], dh_sem.at[t % 2])

            fetch(0).start()

            def back(t, _):
                r = pl.ds(pl.multiple_of(t * 256, 256), 256)
                fetch(t).wait()
                pl.when(t + 1 < n // 256)(lambda: fetch(t + 1).start())
                da = da_s[r, :].astype(BF).astype(F32)
                wide = h_s[t % 2].astype(F32)
                s = norm_scale(wide)
                dx = s * (da - wide * (s * s * jnp.mean(da * wide, -1, keepdims=True)))
                pl.when(t >= 2)(lambda: store(t - 2).wait())
                dh_s[t % 2] = (dy_ref[r, :].astype(F32) + dx.astype(BF).astype(F32)).astype(BF)
                store(t).start()
                return 0

            lax.fori_loop(0, n // 256, back, 0)
            pair_last(steps - 3)
            pair_last(steps - 2)
            store(n // 256 - 2).wait()
            store(n // 256 - 1).wait()
            wait(left_copies(False))
            squares = squares_of(gate_ref[:, :most], up_ref[:, :most], down_ref[...])
            squares_ref[...] = jnp.full(squares_ref.shape, squares, F32)
            return
        pair_first(steps - 1)
        pair_second(steps - 2)
        pair_last(steps - 3)
        known = before_ref[...] + squares_of(gate1_out[:, most:], up1_out[:, most:], down_ref[...])
        pair_second(steps - 1)
        pair_last(steps - 2)
        pair_last(steps - 1)
        sq_s[...] = known + squares_of(gate_ref[...], up_ref[...])
        copies = [send(sq_s, sq_in.at[k], (sq_sem.at[0, k], sq_sem.at[1, k]), other(k)) for k in range(1, 8)]
        start(copies)
        wait(copies)
        sq_in[0] = sq_s[...]
        parts_of = [sq_in[k] for k in range(8)]
        while len(parts_of) > 1:
            parts_of = [one + two for one, two in zip(parts_of[::2], parts_of[1::2], strict=True)]
        squares_ref[...] = parts_of[0]


def backward(number, a, dy, act, sa, sb, weights, h=None, after=None, tokens=512, tile=512):
    wg, wu, wd = weights
    n, d = a.shape
    ff = act.shape[1]
    parts, steps, states = n // tokens, ff // tile, h is not None
    column = lambda i: jnp.maximum(i - 4, 0) // parts
    part = lambda i: jnp.maximum(i - 4, 0) % parts
    saved = pl.BlockSpec((tokens, tile), lambda i: (part(i), column(i)))
    rows_of = pl.BlockSpec((None, tile, d), lambda i: (number, column(i), 0))
    columns_of = pl.BlockSpec((None, d, tile), lambda i: (number, 0, column(i)))
    anywhere = pl.BlockSpec(memory_space=pl.ANY)
    dma = pltpu.SemaphoreType.DMA
    v = lambda *shape: pltpu.VMEM(shape, BF)
    f = lambda *shape: pltpu.VMEM(shape, F32)
    r, q, p = ff // 8, ff // 16, d // 8
    units = steps if states else steps + 1
    down_scratch = [v(2, 2, r, d)] * 3 + [f(2, q, d)] * 2 + [v(2, q, d)] * 4 + [v(q, d)] * 4
    pair_scratch = [v(2, 2, p, tile)] * 2 + [v(2, 2, 2, p, tile), f(3, 2, p, tile)]
    pair_scratch += [v(2, 2, p, tile), v(units, 2, p, tile), v(2, p, tile), v(units, p, tile)]
    sems = [dma((2, 4)), dma((2, 4)), dma((2, 2, 2)), dma((2, 4, units)), dma((4,))]
    left = sds((4, 2, 2, p, tile), BF)
    if states:
        more, more_specs = [h, wg, wu], [anywhere, columns_of, columns_of]
        also, also_specs = [sds((n, d), BF), left], [anywhere, anywhere]
        scratch = [f(n, d), v(2, 256, d), v(2, 256, d), dma((2,)), dma((2,))]
    else:
        more, more_specs = list(after), [whole((8, 128)), anywhere, whole((p, ff)), whole((p, ff))]
        also, also_specs = [sds((p, ff), BF)] * 2, [whole((p, ff))] * 2
        scratch = [f(8, 128), f(8, 8, 128), dma((2, 8))]
    return pl.pallas_call(
        functools.partial(backward_kernel, states, tokens, tile, steps),
        grid=(4 + steps * parts,),
        in_specs=[whole((n, d)), whole((n, d)), anywhere, saved, saved, rows_of] + more_specs,
        out_specs=[whole((p, ff)), whole((p, ff)), whole((r, d)), whole((8, 128))] + also_specs,
        out_shape=[sds((p, ff), BF), sds((p, ff), BF), sds((r, d), BF), sds((8, 128), F32)] + also,
        scratch_shapes=[v(n, tile)] * 2
        + [v(2, n, ff // 4), dma((2,))]
        + down_scratch
        + pair_scratch * 2
        + sems
        + scratch,
        compiler_params=pltpu.CompilerParams(
            vmem_limit_bytes=VMEM, collective_id=number, has_side_effects=True
        ),
        cost_estimate=cost(6 if states else 4, n, d, ff, 12 * n * ff),
        name="backward",
    )(a, dy, act, sa, sb, wd, *more)


def swap(value, bit):
    return lax.ppermute(value, "dp", [(i, i ^ bit) for i in range(8)])


def adamw_kernel(count, me_ref, squares_ref, g0_ref, g1_ref, w_ref, m_ref, v_ref, wo_ref, mo_ref, vo_ref):
    factor = jnp.minimum(1.0, 0.5 * lax.rsqrt(squares_ref[0:1, 0:1] / count + 1e-30))
    g = jnp.where(pl.program_id(0) == 0, g0_ref[...].astype(F32), g1_ref[...].astype(F32)) * factor
    m = 0.9 * m_ref[...] + 0.1 * g
    v = 0.95 * v_ref[...] + 0.05 * g * g
    step = m * lax.rsqrt(v + 1e-8) + 0.1 * w_ref[...].astype(F32)
    wo_ref[...] = (w_ref[...].astype(F32) - 0.02 * step).astype(BF)
    mo_ref[...], vo_ref[...] = m, v


def adamw(me, squares, count, g0, g1, w, m, v):
    _, rows, columns = m.shape
    by_columns = rows < 128
    block = (rows, columns // PARTS) if by_columns else (rows // PARTS, columns)
    at = (lambda c: (0, c)) if by_columns else (lambda c: (c, 0))
    grad = pl.BlockSpec(block, lambda l, c, s: at(c))
    state = pl.BlockSpec((None, *block), lambda l, c, s: (l, *at(c)))
    mine = (lambda l, c, s: (l, s[0], c)) if by_columns else (lambda l, c, s: (l, s[0] * PARTS + c, 0))
    return pl.pallas_call(
        functools.partial(adamw_kernel, count),
        grid_spec=pltpu.PrefetchScalarGridSpec(
            num_scalar_prefetch=1,
            grid=(2, PARTS),
            in_specs=[whole((8, 128)), grad, grad, pl.BlockSpec((None, *block), mine), state, state],
            out_specs=[state] * 3,
        ),
        out_shape=[sds(m.shape, BF), sds(m.shape, F32), sds(m.shape, F32)],
        compiler_params=params(),
        cost_estimate=pl.CostEstimate(flops=m.size * 4000, bytes_accessed=m.size * 22, transcendentals=0),
        name="adamw",
    )(me, squares, g0, g1, w, m, v)


def place_kernel(pieces, *refs):
    refs = list(refs)
    blocks, out = refs[: len(pieces)], refs[-3]
    buffer, sems = refs[-2], refs[-1]
    (x, y, core), _ = peers()
    todo = []
    at = 0
    for (bit, off), block in zip(pieces, blocks, strict=True):
        rows = block.shape[1]
        slot = 4 * xor(x, bit // 4) + 2 * xor(y, bit // 2 % 2) + xor(core, bit % 2)
        for number in range(block.shape[0]):
            k = len(todo)
            held = buffer.at[pl.ds(at, rows)]
            at += rows
            todo.append(
                (
                    pltpu.make_async_copy(block.at[number], held, sems.at[0, k]),
                    pltpu.make_async_copy(held, out.at[number, slot, pl.ds(off, rows)], sems.at[1, k]),
                )
            )
    for fetch, _ in todo:
        fetch.start()
    for fetch, store in todo:
        fetch.wait()
        store.start()
    for _, store in todo:
        store.wait()


def place(pieces, blocks, into=None, shape=None):
    layers, columns = blocks[0].shape[0], blocks[0].shape[2]
    anywhere = pl.BlockSpec(memory_space=pl.ANY)
    total_rows = layers * sum(b.shape[1] for b in blocks)
    size = 4 * total_rows * columns
    return pl.pallas_call(
        functools.partial(place_kernel, pieces),
        in_specs=[anywhere] * (len(blocks) + (into is not None)),
        out_specs=anywhere,
        out_shape=sds(shape, BF),
        scratch_shapes=[pltpu.VMEM((total_rows, columns), BF), pltpu.SemaphoreType.DMA((2, layers * len(blocks)))],
        input_output_aliases={len(blocks): 0} if into is not None else {},
        compiler_params=params(),
        cost_estimate=pl.CostEstimate(flops=size * 300, bytes_accessed=size, transcendentals=0),
        name="place",
    )(*blocks, *([into] if into is not None else []))


def all_gather(mine):
    done = []
    for w in mine:
        half = w.shape[1] // 32 * 16
        bx, by, bc = (swap(w, bit) for bit in (X, Y, CORE))
        fa = swap(bx[:, :half], Y)
        fb = swap(by[:, half:], X)
        cx, cy = (swap(t, CORE) for t in (bx, by))
        shape = (w.shape[0], 8, *w.shape[1:])
        near = ((0, 0), (1, 0), (4, 0), (5, 0), (2, 0), (3, 0))
        out = place(near, (w, bc, bx, cx, by, cy), None, shape)
        ca, cb = (swap(t, CORE) for t in (fa, fb))
        rest = ((6, 0), (7, 0), (6, half), (7, half))
        out = place(rest, (fa, ca, fb, cb), out, shape)
        done.append(out.reshape(w.shape[0], -1, w.shape[2]))
    return done


def solution(mesh):
    def step(x, dy, *arrays):
        weights, ms, vs = (arrays[i : i + 3] for i in (0, 3, 6))
        h0, dy = x[0], dy[0]
        me = lax.axis_index("dp").astype(jnp.int32).reshape(1)
        a0, act0, sa0, sb0, h1 = forward(0, h0, weights, True)
        a1, act1, sa1, sb1 = forward(1, h1, weights, False)
        gate1, up1, down1, squares, dh1, left = backward(1, a1, dy, act1, sa1, sb1, weights, h1)
        after = (squares, left, gate1, up1)
        *first, squares, gate1, up1 = backward(0, a0, dh1, act0, sa0, sb0, weights, after=after, tokens=1024)
        second = (gate1, up1, down1)
        count = sum(w.size for w in weights)
        new = [adamw(me, squares, count, *args) for args in zip(first, second, weights, ms, vs, strict=True)]
        whole_weights = all_gather([w for w, _, _ in new])
        return (*whole_weights, *(m for _, m, _ in new), *(v for _, _, v in new))

    batch, rows = P(("rep", "dp")), P(None, "dp")
    return jax.shard_map(
        step,
        mesh=mesh,
        in_specs=(batch,) * 2 + (P(),) * 3 + (rows,) * 6,
        out_specs=(P("rep"),) * 3 + (P("rep", "dp"),) * 6,
        check_vma=False,
    )
```

```python
import functools

import jax
import jax.numpy as jnp
from jax import lax
from jax.experimental import pallas as pl
from jax.experimental.pallas import tpu as pltpu
from jax.sharding import PartitionSpec as P


F32, BF = jnp.float32, jnp.bfloat16
VMEM = 67043328
X, Y, CORE = 4, 2, 1
PARTS = 2


def dot(a, b, ca=1, cb=0):
    return lax.dot_general(a, b, (((ca,), (cb,)), ((), ())), preferred_element_type=F32)


def norm_scale(wide):
    return lax.rsqrt(jnp.mean(wide * wide, -1, keepdims=True) + 1e-6)


def whole(shape):
    return pl.BlockSpec(shape, lambda i, *_: (0,) * len(shape), pipeline_mode=pl.Buffered(1))


def sds(shape, dtype):
    return jax.ShapeDtypeStruct(shape, dtype)


def params():
    return pltpu.CompilerParams(vmem_limit_bytes=VMEM)


def cost(matmuls, n, d, ff, bytes_accessed):
    return pl.CostEstimate(flops=2 * matmuls * n * d * ff, bytes_accessed=bytes_accessed, transcendentals=0)


def forward_kernel(chunk, down, h_ref, wg_ref, wu_ref, *refs):
    if down:
        wd_ref, a_ref, act_ref, sa_ref, sb_ref, h1_ref = refs
    else:
        a_ref, act_ref, sa_ref, sb_ref = refs
    wide = h_ref[...].astype(F32)
    a = (wide * norm_scale(wide)).astype(BF)
    a_ref[...] = a
    for c in range(wg_ref.shape[1] // chunk):
        s = pl.ds(c * chunk, chunk)
        gate, up = dot(a, wg_ref[:, s]), dot(a, wu_ref[:, s])
        sig = 1.0 / (1.0 + jnp.exp(-gate))
        silu = gate * sig
        act_ref[:, s] = (silu * up).astype(BF)
        sb_ref[:, s] = silu
        sa_ref[:, s] = up * (sig + silu * (1.0 - sig))
    if down:
        out = dot(act_ref[...], wd_ref[...]).astype(BF)
        h1_ref[...] = (h_ref[...].astype(F32) + out.astype(F32)).astype(BF)


def forward(number, h, weights, down, tile=256, chunk=1280):
    n, d = h.shape
    ff = weights[0].shape[2]
    row = lambda w: pl.BlockSpec((tile, w), lambda i: (i, 0))
    of = lambda w: pl.BlockSpec((None, *w.shape[1:]), lambda i: (number, 0, 0), pipeline_mode=pl.Buffered(1))
    used = weights[: 2 + down]
    return pl.pallas_call(
        functools.partial(forward_kernel, chunk, down),
        grid=(n // tile,),
        in_specs=[row(d)] + [of(w) for w in used],
        out_specs=[row(d), row(ff), row(ff), row(ff)] + [row(d)] * down,
        out_shape=[sds((n, d), BF), sds((n, ff), BF), sds((n, ff), F32), sds((n, ff), F32)] + [sds((n, d), BF)] * down,
        compiler_params=params(),
        cost_estimate=cost(3 if down else 2, n, d, ff, 10 * n * ff),
        name="forward",
    )(h, *used)


def peers():
    me = lax.axis_index("dp")
    x, y, core = me // 4, me // 2 % 2, me % 2
    return (x, y, core), (me + 1 - 2 * core, me + 2 - 4 * y, me + 4 - 8 * x)


def xor(a, b):
    return a + b - 2 * a * b


def send(src, dst, sems, to):
    return pltpu.make_async_remote_copy(
        src_ref=src,
        dst_ref=dst,
        send_sem=sems[0],
        recv_sem=sems[1],
        device_id={"dp": to},
        device_id_type=pl.DeviceIdType.MESH,
    )


def total(*terms):
    return sum(t.astype(F32) for t in terms)


def backward_kernel(states, tokens, tile, steps, *refs):
    refs = list(refs)
    take = lambda k: [refs.pop(0) for _ in range(k)]
    a_ref, dy_ref, act_ref, sa_ref, sb_ref, wd_ref = take(6)
    if states:
        h_ref, wg_ref, wu_ref = take(3)
    else:
        before_ref, left_ref, gate1_ref, up1_ref = take(4)
    gate_ref, up_ref, down_ref, squares_ref = take(4)
    if states:
        dh_ref, left_ref = take(2)
    else:
        gate1_out, up1_out = take(2)
    act_s, act_sem = take(2)
    dg_s, du_s = (act_s.at[k, :, pl.ds(0, tile)] for k in (0, 1))
    dk, do, di, da_sum, db_sum, dsx, dsy, drx, dry, dsy2, dsx2, dry2, drx2 = take(13)
    gk, go, gi, g_sum, gs1, gr1, gs2, gr2 = take(8)
    uk, uo, ui, u_sum, us1, ur1, us2, ur2 = take(8)
    d_core, d_link, p_core, p_link, left_sem = take(5)
    if states:
        da_s, h_s, dh_s, h_sem, dh_sem = take(5)
    else:
        sq_s, sq_in, sq_sem = take(3)

    n, d = a_ref.shape
    parts = n // tokens
    i = pl.program_id(0)
    (x, y, core), (to_core, to_y, to_x) = peers()
    mine = core == 0

    def other(k):
        return 4 * xor(x, k // 4) + 2 * xor(y, k // 2 % 2) + xor(core, k % 2)

    def start(copies):
        for c in copies:
            c.start()

    def wait(copies):
        for c in copies:
            c.wait()

    def down_copy(k):
        slot = 1 - k // 2, 1 - k % 2
        return send(do.at[slot], di.at[slot], (d_core.at[0, k], d_core.at[1, k]), to_core)

    def fetch_act(k):
        width = act_ref.shape[1] // 4
        q = 2 * xor(1 - k // 2, x) + xor(1 - k % 2, y)
        columns = pl.ds(pl.multiple_of(q * width, 128), width)
        return pltpu.make_async_copy(act_ref.at[:, columns], act_s.at[k % 2], act_sem.at[k % 2])

    def down_links(stage, way):
        sem = lambda k: (d_link.at[0, k], d_link.at[1, k])
        if stage == 1:
            return send(dsx, drx, sem(0), to_x) if way == "x" else send(dsy, dry, sem(1), to_y)
        return send(dsx2, drx2, sem(3), to_x) if way == "x" else send(dsy2, dry2, sem(2), to_y)

    def core_copy(which, u):
        src, dst = ((go, gi), (uo, ui))[which]
        slot = u % 2
        return send(src, dst.at[slot], (p_core.at[0, which, slot], p_core.at[1, which, slot]), to_core)

    def pair_links(stage, u):
        sem = lambda k: (p_link.at[0, k, u], p_link.at[1, k, u])
        slot = u % 2
        if stage == 1:
            return send(gs1.at[slot], gr1.at[u], sem(0), to_x), send(us1.at[slot], ur1.at[u], sem(1), to_y)
        return send(gs2.at[slot], gr2.at[u], sem(2), to_y), send(us2.at[slot], ur2.at[u], sem(3), to_x)

    half = dk.shape[2] // 2
    lo, hi = pl.ds(0, half), pl.ds(half, half)

    def down_x():
        wait([down_copy(0), down_copy(1)])
        dsx[...] = total(dk[1, :, lo], di[1, :, lo]).astype(BF)
        down_links(1, "x").start()

    def down_y():
        wait([down_copy(2)])
        dsy[...] = total(dk[:, 1, hi], di[:, 1, hi]).astype(BF)
        down_links(1, "y").start()

    def down_sums():
        wait([down_copy(3)])
        da_sum[...] = total(dk[0, :, lo], di[0, :, lo])
        db_sum[...] = total(dk[:, 0, hi], di[:, 0, hi])

    def down_second():
        down_links(1, "x").wait()
        dsy2[...] = total(da_sum[1], drx[1]).astype(BF)
        down_links(2, "y").start()
        da_sum[0] = total(da_sum[0], drx[0])
        down_links(1, "y").wait()
        dsx2[...] = total(db_sum[1], dry[1]).astype(BF)
        down_links(2, "x").start()
        db_sum[0] = total(db_sum[0], dry[0])

    def down_last():
        down_links(2, "y").wait()
        down_links(2, "x").wait()
        down_ref[lo, :] = total(da_sum[0], dry2[...]).astype(BF)
        down_ref[hi, :] = total(db_sum[0], drx2[...]).astype(BF)

    def pair_first(u):
        slot, held = u % 2, u % 3
        wait([core_copy(0, u), core_copy(1, u)])
        gs1[slot] = total(gk[1], gi[slot, 1]).astype(BF)
        us1[slot] = total(uk[:, 1], ui[slot, :, 1]).astype(BF)
        start(pair_links(1, u))
        g_sum[held] = total(gk[0], gi[slot, 0])
        u_sum[held] = total(uk[:, 0], ui[slot, :, 0])

    def pair_second(u):
        slot, held = u % 2, u % 3
        wait(pair_links(1, u))
        gs2[slot] = total(g_sum[held, 1], gr1[u, 1]).astype(BF)
        us2[slot] = total(u_sum[held, 1], ur1[u, 1]).astype(BF)
        start(pair_links(2, u))
        g_sum[held, 0] = total(g_sum[held, 0], gr1[u, 0])
        u_sum[held, 0] = total(u_sum[held, 0], ur1[u, 0])

    def pair_last(u, gate_to=None, up_to=None, column=None):
        held = u % 3
        wait(pair_links(2, u))
        column = u if column is None else column
        cols = pl.ds(pl.multiple_of(column * tile, tile), tile)
        gate_to, up_to = (gate_ref, up_ref) if gate_to is None else (gate_to, up_to)
        gate_to[:, cols] = total(g_sum[held, 0], gr2[u]).astype(BF)
        up_to[:, cols] = total(u_sum[held, 0], ur2[u]).astype(BF)

    def left_copies(fill):
        held = (gk, go, uk, uo)
        ends = [(left_ref.at[k], t) if fill else (t, left_ref.at[k]) for k, t in enumerate(held)]
        return [pltpu.make_async_copy(src, dst, left_sem.at[k]) for k, (src, dst) in enumerate(ends)]

    def squares_of(*values):
        return sum(jnp.sum(jnp.square(value.astype(F32))) for value in values)

    given = steps
    most = (steps - 1) * tile

    @pl.when(i == 0)
    def _():
        fetch_act(0).start()
        fetch_act(1).start()
        if not states:
            start(left_copies(True))
        barrier = pltpu.get_barrier_semaphore()
        met = (to_core, to_y, to_x) if states else [other(k) for k in range(1, 8)]
        for to in met:
            pl.semaphore_signal(barrier, inc=1, device_id={"dp": to}, device_id_type=pl.DeviceIdType.MESH)
        pl.semaphore_wait(barrier, len(met))
        if states:

            def clear(t, _):
                da_s[pl.ds(pl.multiple_of(t * 256, 256), 256), :] = jnp.zeros((256, d), F32)
                return 0

            lax.fori_loop(0, n // 256, clear, 0)
        else:
            wait(left_copies(True))
            core_copy(0, given).start()
            core_copy(1, given).start()
            gate1_out[:, :most] = gate1_ref[:, :most]
            up1_out[:, :most] = up1_ref[:, :most]

    @pl.when(i < 4)
    def _():
        fetch_act(i).wait()
        g = dot(act_s[i % 2], dy_ref[...], 0, 0)
        rows = g.shape[0] // 2
        sx, sy = 1 - i // 2, 1 - i % 2
        dk[sx, sy] = jnp.where(mine, g[:rows], g[rows:]).astype(BF)
        do[sx, sy] = jnp.where(mine, g[rows:], g[:rows]).astype(BF)
        down_copy(i).start()
        pl.when(i < 2)(lambda: fetch_act(i + 2).start())
        if not states:
            pl.when(i == 1)(lambda: pair_first(given))
            pl.when(i == 3)(lambda: pair_second(given))
        pl.when(i == 2)(down_x)
        pl.when(i == 3)(down_y)

    @pl.when(i >= 4)
    def _():
        j, t = (i - 4) // parts, (i - 4) % parts
        r = pl.ds(pl.multiple_of(t * tokens, tokens), tokens)
        dp = dot(dy_ref[r, :], wd_ref[...], 1, 1).astype(BF).astype(F32)
        du = (dp * sb_ref[...]).astype(BF)
        dg = (dp * sa_ref[...]).astype(BF)
        dg_s[r, :], du_s[r, :] = dg, du
        if states:
            da_s[r, :] += dot(dg, wg_ref[...], 1, 1) + dot(du, wu_ref[...], 1, 1)

        @pl.when(t == parts - 1)
        def _():
            pl.when(j == 0)(down_sums)
            pl.when(j >= 1)(lambda: pair_first(j - 1))
            pl.when(j == 1)(down_second)
            pl.when(j >= 2)(lambda: pair_second(j - 2))
            if not states:
                pl.when(j == 1)(lambda: pair_last(given, gate1_out, up1_out, steps - 1))
            pl.when(j == 2)(down_last)
            pl.when(j >= 3)(lambda: pair_last(j - 3))
            rows = d // 8
            for which, (by, keep, out) in enumerate(((dg_s, gk, go), (du_s, uk, uo))):
                g = dot(a_ref[...], by[...], 0, 0)
                for q in range(4):
                    first, second = (g[(2 * q + e) * rows : (2 * q + e + 1) * rows] for e in (0, 1))
                    sx, sy = xor(q // 2, x), xor(q % 2, y)
                    keep[sx, sy] = jnp.where(mine, first, second).astype(BF)
                    out[sx, sy] = jnp.where(mine, second, first).astype(BF)
                if states:
                    pl.when(j < steps - 1)(lambda: core_copy(which, j).start())
                else:
                    core_copy(which, j).start()

    @pl.when(i == 4 + steps * parts - 1)
    def _():
        if states:
            start(left_copies(False))
            few, slots = h_s.shape[1], h_s.shape[0]

            def fetch(t):
                rows = pl.ds(pl.multiple_of(t * few, few), few)
                return pltpu.make_async_copy(h_ref.at[rows, :], h_s.at[t % slots], h_sem.at[t % slots])

            def store(t):
                rows = pl.ds(pl.multiple_of(t * few, few), few)
                return pltpu.make_async_copy(dh_s.at[t % slots], dh_ref.at[rows, :], dh_sem.at[t % slots])

            for t in range(slots):
                fetch(t).start()
            pair_second(steps - 2)

            def back(t, _):
                r = pl.ds(pl.multiple_of(t * few, few), few)
                fetch(t).wait()
                da = da_s[r, :].astype(BF).astype(F32)
                wide = h_s[t % slots].astype(F32)
                s = norm_scale(wide)
                dx = s * (da - wide * (s * s * jnp.mean(da * wide, -1, keepdims=True)))
                pl.when(t >= slots)(lambda: store(t - slots).wait())
                dh_s[t % slots] = (dy_ref[r, :].astype(F32) + dx.astype(BF).astype(F32)).astype(BF)
                store(t).start()
                pl.when(t + slots < n // few)(lambda: fetch(t + slots).start())
                return 0

            lax.fori_loop(0, n // few, back, 0)
            pair_last(steps - 3)
            pair_last(steps - 2)
            for t in range(slots):
                store(n // few - slots + t).wait()
            wait(left_copies(False))
            squares = squares_of(gate_ref[:, :most], up_ref[:, :most], down_ref[...])
            squares_ref[...] = jnp.full(squares_ref.shape, squares, F32)
            return
        pair_first(steps - 1)
        pair_second(steps - 2)
        pair_last(steps - 3)
        known = before_ref[...] + squares_of(gate1_out[:, most:], up1_out[:, most:], down_ref[...])
        pair_second(steps - 1)
        pair_last(steps - 2)
        pair_last(steps - 1)
        sq_s[...] = known + squares_of(gate_ref[...], up_ref[...])
        copies = [send(sq_s, sq_in.at[k], (sq_sem.at[0, k], sq_sem.at[1, k]), other(k)) for k in range(1, 8)]
        start(copies)
        wait(copies)
        sq_in[0] = sq_s[...]
        parts_of = [sq_in[k] for k in range(8)]
        while len(parts_of) > 1:
            parts_of = [one + two for one, two in zip(parts_of[::2], parts_of[1::2], strict=True)]
        squares_ref[...] = parts_of[0]


def backward(number, a, dy, act, sa, sb, weights, h=None, after=None, tokens=512, tile=512):
    wg, wu, wd = weights
    n, d = a.shape
    ff = act.shape[1]
    parts, steps, states = n // tokens, ff // tile, h is not None
    column = lambda i: jnp.maximum(i - 4, 0) // parts
    part = lambda i: jnp.maximum(i - 4, 0) % parts
    saved = pl.BlockSpec((tokens, tile), lambda i: (part(i), column(i)))
    rows_of = pl.BlockSpec((None, tile, d), lambda i: (number, column(i), 0))
    columns_of = pl.BlockSpec((None, d, tile), lambda i: (number, 0, column(i)))
    anywhere = pl.BlockSpec(memory_space=pl.ANY)
    dma = pltpu.SemaphoreType.DMA
    v = lambda *shape: pltpu.VMEM(shape, BF)
    f = lambda *shape: pltpu.VMEM(shape, F32)
    r, q, p = ff // 8, ff // 16, d // 8
    units = steps - 1 if states else steps + 1
    down_scratch = [v(2, 2, r, d)] * 3 + [f(2, q, d)] * 2 + [v(2, q, d)] * 4 + [v(q, d)] * 4
    pair_scratch = [v(2, 2, p, tile)] * 2 + [v(2, 2, 2, p, tile), f(3, 2, p, tile)]
    pair_scratch += [v(2, 2, p, tile), v(units, 2, p, tile), v(2, p, tile), v(units, p, tile)]
    sems = [dma((2, 4)), dma((2, 4)), dma((2, 2, 2)), dma((2, 4, units)), dma((4,))]
    left = sds((4, 2, 2, p, tile), BF)
    if states:
        more, more_specs = [h, wg, wu], [anywhere, columns_of, columns_of]
        also, also_specs = [sds((n, d), BF), left], [anywhere, anywhere]
        scratch = [f(n, d), v(4, 128, d), v(4, 128, d), dma((4,)), dma((4,))]
    else:
        more, more_specs = list(after), [whole((8, 128)), anywhere, whole((p, ff)), whole((p, ff))]
        also, also_specs = [sds((p, ff), BF)] * 2, [whole((p, ff))] * 2
        scratch = [f(8, 128), f(8, 8, 128), dma((2, 8))]
    return pl.pallas_call(
        functools.partial(backward_kernel, states, tokens, tile, steps),
        grid=(4 + steps * parts,),
        in_specs=[whole((n, d)), whole((n, d)), anywhere, saved, saved, rows_of] + more_specs,
        out_specs=[whole((p, ff)), whole((p, ff)), whole((r, d)), whole((8, 128))] + also_specs,
        out_shape=[sds((p, ff), BF), sds((p, ff), BF), sds((r, d), BF), sds((8, 128), F32)] + also,
        scratch_shapes=[v(2, n, max(tile, ff // 4)), dma((2,))]
        + down_scratch
        + pair_scratch * 2
        + sems
        + scratch,
        compiler_params=pltpu.CompilerParams(
            vmem_limit_bytes=VMEM, collective_id=number, has_side_effects=True
        ),
        cost_estimate=cost(6 if states else 4, n, d, ff, 12 * n * ff),
        name="backward",
    )(a, dy, act, sa, sb, wd, *more)


def swap(value, bit):
    return lax.ppermute(value, "dp", [(i, i ^ bit) for i in range(8)])


def adamw_kernel(count, me_ref, squares_ref, g0_ref, g1_ref, w_ref, m_ref, v_ref, wo_ref, mo_ref, vo_ref):
    factor = jnp.minimum(1.0, 0.5 * lax.rsqrt(squares_ref[0:1, 0:1] / count + 1e-30))
    g = jnp.where(pl.program_id(0) == 0, g0_ref[...].astype(F32), g1_ref[...].astype(F32)) * factor
    m = 0.9 * m_ref[...] + 0.1 * g
    v = 0.95 * v_ref[...] + 0.05 * g * g
    step = m * lax.rsqrt(v + 1e-8) + 0.1 * w_ref[...].astype(F32)
    wo_ref[...] = (w_ref[...].astype(F32) - 0.02 * step).astype(BF)
    mo_ref[...], vo_ref[...] = m, v


def adamw(me, squares, count, g0, g1, w, m, v):
    _, rows, columns = m.shape
    by_columns = rows < 128
    block = (rows, columns // PARTS) if by_columns else (rows // PARTS, columns)
    at = (lambda c: (0, c)) if by_columns else (lambda c: (c, 0))
    grad = pl.BlockSpec(block, lambda l, c, s: at(c))
    state = pl.BlockSpec((None, *block), lambda l, c, s: (l, *at(c)))
    mine = (lambda l, c, s: (l, s[0], c)) if by_columns else (lambda l, c, s: (l, s[0] * PARTS + c, 0))
    return pl.pallas_call(
        functools.partial(adamw_kernel, count),
        grid_spec=pltpu.PrefetchScalarGridSpec(
            num_scalar_prefetch=1,
            grid=(2, PARTS),
            in_specs=[whole((8, 128)), grad, grad, pl.BlockSpec((None, *block), mine), state, state],
            out_specs=[state] * 3,
        ),
        out_shape=[sds(m.shape, BF), sds(m.shape, F32), sds(m.shape, F32)],
        compiler_params=params(),
        cost_estimate=pl.CostEstimate(flops=m.size * 4000, bytes_accessed=m.size * 22, transcendentals=0),
        name="adamw",
    )(me, squares, g0, g1, w, m, v)


def place_kernel(pieces, *refs):
    refs = list(refs)
    blocks, out = refs[: len(pieces)], refs[-3]
    buffer, sems = refs[-2], refs[-1]
    (x, y, core), _ = peers()
    todo = []
    at = 0
    for (bit, off), block in zip(pieces, blocks, strict=True):
        rows = block.shape[1]
        slot = 4 * xor(x, bit // 4) + 2 * xor(y, bit // 2 % 2) + xor(core, bit % 2)
        for number in range(block.shape[0]):
            k = len(todo)
            held = buffer.at[pl.ds(at, rows)]
            at += rows
            todo.append(
                (
                    pltpu.make_async_copy(block.at[number], held, sems.at[0, k]),
                    pltpu.make_async_copy(held, out.at[number, slot, pl.ds(off, rows)], sems.at[1, k]),
                )
            )
    for fetch, _ in todo:
        fetch.start()
    for fetch, store in todo:
        fetch.wait()
        store.start()
    for _, store in todo:
        store.wait()


def place(pieces, blocks, into=None, shape=None):
    layers, columns = blocks[0].shape[0], blocks[0].shape[2]
    anywhere = pl.BlockSpec(memory_space=pl.ANY)
    total_rows = layers * sum(b.shape[1] for b in blocks)
    size = 4 * total_rows * columns
    return pl.pallas_call(
        functools.partial(place_kernel, pieces),
        in_specs=[anywhere] * (len(blocks) + (into is not None)),
        out_specs=anywhere,
        out_shape=sds(shape, BF),
        scratch_shapes=[pltpu.VMEM((total_rows, columns), BF), pltpu.SemaphoreType.DMA((2, layers * len(blocks)))],
        input_output_aliases={len(blocks): 0} if into is not None else {},
        compiler_params=params(),
        cost_estimate=pl.CostEstimate(flops=size * 300, bytes_accessed=size, transcendentals=0),
        name="place",
    )(*blocks, *([into] if into is not None else []))


def all_gather(mine):
    done = []
    for k, w in enumerate(mine):
        half = (w.shape[1] + 16 * (k % 2)) // 32 * 16
        bx, by, bc = (swap(w, bit) for bit in (X, Y, CORE))
        fa = swap(bx[:, :half], Y)
        fb = swap(by[:, half:], X)
        cx, cy = (swap(t, CORE) for t in (bx, by))
        shape = (w.shape[0], 8, *w.shape[1:])
        near = ((0, 0), (1, 0), (4, 0), (5, 0), (2, 0), (3, 0))
        out = place(near, (w, bc, bx, cx, by, cy), None, shape)
        ca, cb = (swap(t, CORE) for t in (fa, fb))
        rest = ((6, 0), (7, 0), (6, half), (7, half))
        out = place(rest, (fa, ca, fb, cb), out, shape)
        done.append(out.reshape(w.shape[0], -1, w.shape[2]))
    return done


def solution(mesh):
    def step(x, dy, *arrays):
        weights, ms, vs = (arrays[i : i + 3] for i in (0, 3, 6))
        h0, dy = x[0], dy[0]
        me = lax.axis_index("dp").astype(jnp.int32).reshape(1)
        a0, act0, sa0, sb0, h1 = forward(0, h0, weights, True)
        a1, act1, sa1, sb1 = forward(1, h1, weights, False)
        gate1, up1, down1, squares, dh1, left = backward(1, a1, dy, act1, sa1, sb1, weights, h1, tokens=512)
        after = (squares, left, gate1, up1)
        *first, squares, gate1, up1 = backward(0, a0, dh1, act0, sa0, sb0, weights, after=after, tokens=1024)
        second = (gate1, up1, down1)
        count = sum(w.size for w in weights)
        new = [adamw(me, squares, count, *args) for args in zip(first, second, weights, ms, vs, strict=True)]
        whole_weights = all_gather([w for w, _, _ in new])
        return (*whole_weights, *(m for _, m, _ in new), *(v for _, _, v in new))

    batch, rows = P(("rep", "dp")), P(None, "dp")
    return jax.shard_map(
        step,
        mesh=mesh,
        in_specs=(batch,) * 2 + (P(),) * 3 + (rows,) * 6,
        out_specs=(P("rep"),) * 3 + (P("rep", "dp"),) * 6,
        check_vma=False,
    )
```
